512 devices in a mesh: lon: 32 (over x_hi, z), lat: 16 (over x_lo, y, core).
Axes of the slice: x: 4 (x_hi: 2, x_lo: 2; x = x_hi * 2 + x_lo), y: 4, z: 16, core: 2. Of those that a mesh axis runs over, the one named last changes fastest.
Arguments:
- tracers: float32 [40, 8, 128, 4096], P(None, None, 'lat', 'lon'), may hold values from -6 to 6
- kmt: int32 [128, 4096], P('lat', 'lon'), may hold values from 0 to 8
Outputs:
- updated: float32 [40, 8, 128, 4096], P(None, None, 'lat', 'lon')
The draws below stay inside these ranges and needn't reach their ends.
Inputs may be any that keep to these rules, and one draw needn't show every extreme that they name: Level k of column (j, i) is ocean exactly when k < kmt[j, i].
All inputs are finite; a program needn't handle non-finite values.
Results may differ from the reference program's by a relative error of at most 0.00002.
Values sent between devices are 32-bit elements; how exact they have to be, the bound alone decides.
A program may use at most 64 MiB of HBM per device.

```python
import jax
import jax.numpy as jnp
from jax import lax

NTRAC = 40
NZ = 8
NY = 128
NX = 4096


def with_ends(array, rng, least, largest):
    longest = array.shape.index(max(array.shape))
    spots = []
    for shift in (0, 1):
        where = [jax.random.randint(jax.random.fold_in(rng, axis), (), 0, length) for axis, length in enumerate(array.shape)]
        where[longest] = (where[longest] + shift) % array.shape[longest]
        spots.append(tuple(where))
    return array.at[spots[0]].set(least).at[spots[1]].set(largest)


def block_scale(key, extent, pieces, least, largest):
    level, own = 1.0, jax.random.fold_in(key, 6)
    for dim, blocks in pieces:
        heights = jnp.exp(jax.random.uniform(jax.random.fold_in(own, dim), (blocks,), jnp.float32, least / len(pieces), largest / len(pieces)))
        level = level * jnp.repeat(heights, extent[dim] // blocks).reshape([-1 if axis == dim else 1 for axis in range(len(extent))])
    return level


def normal_values(rng, dims, scale, bound, pieces=(), kind=jnp.bfloat16):
    level = block_scale(rng, dims, pieces, -0.22, 0.18) if pieces else 1.0
    values = jax.random.normal(rng, dims, jnp.float32) * scale * level
    return jnp.minimum(jnp.maximum(values, -bound), bound).astype(kind)


def setup_inputs(seed: int = 0) -> dict:
    streams_of = jax.random.split(jax.random.key(seed), 3)
    tracers = normal_values(streams_of[0], (NTRAC, NZ, NY, NX), 1.0, 6.0, ((2, 16), (3, 32)), jnp.float32)
    kmt = with_ends(jax.random.randint(streams_of[1], (NY, NX), 0, NZ + 1), jax.random.fold_in(streams_of[1], 1), 0, NZ).astype(jnp.int32)
    return dict(tracers=tracers, kmt=kmt)


THERMAL = 0.2
HALINE = 0.8
REDI_COEF = 0.1
SKEW_COEF = 0.05
SLOPE_MAX = 0.6
SLOPE_WIDTH = 0.2


def taper(slope):
    return slope * 0.5 * (1.0 + jnp.tanh((SLOPE_MAX - jnp.abs(slope)) / SLOPE_WIDTH))


def pad_levels(values):
    zero_layer = jnp.zeros_like(values[..., :1, :, :])
    return jnp.concatenate([zero_layer, values, zero_layer], axis=-3)


def slope_fields(density, wet_mask):
    level_mask = wet_mask[1:] * wet_mask[:-1]
    strat = (density[1:] - density[:-1]) * level_mask
    strat_pad = pad_levels(strat)
    strat_cell = 0.5 * (strat_pad[:-1] + strat_pad[1:])
    east_mask = wet_mask[:, 1:-1, :-1] * wet_mask[:, 1:-1, 1:]
    north_mask = wet_mask[:, :-1, 1:-1] * wet_mask[:, 1:, 1:-1]
    grad_east = (density[:, 1:-1, 1:] - density[:, 1:-1, :-1]) * east_mask
    strat_east = 0.5 * (strat_cell[:, 1:-1, 1:] + strat_cell[:, 1:-1, :-1])
    slope_x = taper(grad_east / jnp.maximum(strat_east, 1.0))
    grad_north = (density[:, 1:, 1:-1] - density[:, :-1, 1:-1]) * north_mask
    strat_north = 0.5 * (strat_cell[:, 1:, 1:-1] + strat_cell[:, :-1, 1:-1])
    slope_y = taper(grad_north / jnp.maximum(strat_north, 1.0))
    cell_x = 0.5 * (slope_x[..., :-1] + slope_x[..., 1:])
    cell_y = 0.5 * (slope_y[:, :-1, :] + slope_y[:, 1:, :])
    level_x = 0.5 * (cell_x[:-1] + cell_x[1:])
    level_y = 0.5 * (cell_y[:-1] + cell_y[1:])
    return (level_mask, east_mask, north_mask, slope_x, slope_y, level_x, level_y)


def tracer_step(field, fields):
    level_mask, east_mask, north_mask, slope_x, slope_y, level_x, level_y = fields
    vert_diff = (field[..., 1:, :, :] - field[..., :-1, :, :]) * level_mask
    vert_pad = pad_levels(vert_diff)
    vert_cell = 0.5 * (vert_pad[..., :-1, :, :] + vert_pad[..., 1:, :, :])
    grad_x = (field[..., 1:-1, 1:] - field[..., 1:-1, :-1]) * east_mask
    grad_y = (field[..., 1:, 1:-1] - field[..., :-1, 1:-1]) * north_mask
    flux_x = -(REDI_COEF * grad_x + (REDI_COEF - SKEW_COEF) * slope_x
               * 0.5 * (vert_cell[..., 1:-1, 1:] + vert_cell[..., 1:-1, :-1])) * east_mask
    flux_y = -(REDI_COEF * grad_y + (REDI_COEF - SKEW_COEF) * slope_y
               * 0.5 * (vert_cell[..., 1:, 1:-1] + vert_cell[..., :-1, 1:-1])) * north_mask
    cell_gx = 0.5 * (grad_x[..., :-1] + grad_x[..., 1:])
    cell_gy = 0.5 * (grad_y[..., :-1, :] + grad_y[..., 1:, :])
    level_gx = 0.5 * (cell_gx[..., :-1, :, :] + cell_gx[..., 1:, :, :])
    level_gy = 0.5 * (cell_gy[..., :-1, :, :] + cell_gy[..., 1:, :, :])
    flux_z = -((REDI_COEF + SKEW_COEF) * (level_x * level_gx + level_y * level_gy)
               + REDI_COEF * (level_x * level_x + level_y * level_y) * vert_diff[..., 1:-1, 1:-1]) * level_mask[:, 1:-1, 1:-1]
    flux_pad = pad_levels(flux_z)
    tendency = -((flux_x[..., 1:] - flux_x[..., :-1]) + (flux_y[..., 1:, :] - flux_y[..., :-1, :])
                 + (flux_pad[..., 1:, :, :] - flux_pad[..., :-1, :, :]))
    return field[..., 1:-1, 1:-1] + tendency


def extend(field):
    beside_all = jnp.concatenate([field[..., -1:], field, field[..., :1]], axis=-1)
    north_row = beside_all[..., -1:, ::-1]
    south_row = jnp.zeros_like(beside_all[..., :1, :])
    return jnp.concatenate([south_row, beside_all, north_row], axis=-2)


def reference(tracers, kmt):
    level_index = lax.broadcasted_iota(jnp.int32, (NZ, NY, NX), 0)
    wet_mask = (level_index < kmt[None]).astype(jnp.float32)
    density = HALINE * tracers[1] - THERMAL * tracers[0]
    fields = slope_fields(extend(density), extend(wet_mask))
    return lax.map(lambda single: tracer_step(extend(single), fields), tracers)
```

```python
import functools

import jax
import jax.numpy as jnp
from jax import lax
from jax.experimental import pallas as pl
from jax.experimental.pallas import tpu as pltpu
from jax.sharding import PartitionSpec as P

THERMAL = 0.2
HALINE = 0.8
REDI_COEF = 0.1
SKEW_COEF = 0.05
SLOPE_MAX = 0.6
SLOPE_WIDTH = 0.2
SLOPE_FLUX = (REDI_COEF - SKEW_COEF) * 0.25
CROSS = (REDI_COEF + SKEW_COEF) * 0.25 / REDI_COEF

ROWS = 8
LANES = 128
LEVELS = 8
MESH = pl.DeviceIdType.MESH
VMEM = pltpu.VMEM


def taper(slope):
    return slope * 0.5 * (1.0 + jnp.tanh((SLOPE_MAX - jnp.abs(slope)) / SLOPE_WIDTH))


def slope_of(step, mask, strat_twice):
    return taper(step * mask / jnp.maximum(0.25 * strat_twice, 1.0))


def below(limit, level):
    return jnp.where(level < limit, 1.0, 0.0)


def vertical_pair(values, mask, axis):
    size = values.shape[axis]
    diff = (pltpu.roll(values, size - 1, axis) - values) * mask
    return diff, diff + pltpu.roll(diff, 1, axis)


def up_one(values, axis):
    return pltpu.roll(values, values.shape[axis] - 1, axis)


def kernel(
    channels, chunks, tracers, kmt, out,
    field, row_south, row_inner, row_north, depth,
    from_south, from_north, depth_south, depth_north,
    to_west, to_east, from_west, from_east,
    coef, edge_x, row_coef,
    load_sem, send_sem, recv_sem,
):
    lon, lat = lax.axis_index("lon"), lax.axis_index("lat")
    blocks, bands = lax.axis_size("lon"), lax.axis_size("lat")
    top, bottom = lat == bands - 1, lat == 0
    west = (lax.rem(lon + blocks - 1, blocks), lat)
    east = (lax.rem(lon + 1, blocks), lat)
    north = (jnp.where(top, blocks - 1 - lon, lon), jnp.where(top, lat, lat + 1))
    south = (lon, jnp.maximum(lat - 1, 0))
    groups = to_west.shape[0]
    per_chunk = channels // chunks

    barrier = pltpu.get_barrier_semaphore()
    for other in (north, west, east):
        pl.semaphore_signal(barrier, inc=1, device_id=other, device_id_type=MESH)

    @pl.when(jnp.logical_not(bottom))
    def _():
        pl.semaphore_signal(barrier, inc=1, device_id=south, device_id_type=MESH)

    loads = [
        pltpu.make_async_copy(tracers.at[:, :, ROWS - 1, :], row_north, load_sem.at[0]),
        pltpu.make_async_copy(tracers, field, load_sem.at[1]),
        pltpu.make_async_copy(kmt, depth, load_sem.at[2]),
        pltpu.make_async_copy(tracers.at[:, :, 0, :], row_south, load_sem.at[3]),
        pltpu.make_async_copy(tracers.at[:, :, ROWS - 2, :], row_inner, load_sem.at[4]),
    ]
    for load in loads:
        load.start()
    for load in loads:
        load.wait()

    shape = (ROWS, LANES)
    lane = lax.broadcasted_iota(jnp.int32, shape, 1)
    row = lax.broadcasted_iota(jnp.int32, shape, 0)
    per_group = LANES // LEVELS
    depth_here = depth[...]
    depth_real = depth_here.astype(jnp.float32)

    for side, packed in ((0, to_west), (LANES - 1, to_east)):
        for group in range(groups):
            count = min(per_group, channels - group * per_group)

            def place(slot, total, group=group, side=side):
                piece = jnp.zeros(shape, jnp.float32)
                for level in range(LEVELS):
                    column = field[group * per_group + slot, level]
                    column = pltpu.roll(column, (level - side) % LANES, 1)
                    piece = jnp.where(lane == level, column, piece)
                piece = pltpu.roll(piece, slot * LEVELS, 1)
                return jnp.where(lane // LEVELS == slot, piece, total)

            total = lax.fori_loop(0, count, place, jnp.zeros(shape, jnp.float32))
            if group == groups - 1:
                at = count * LEVELS
                total = jnp.where(lane == at, pltpu.roll(depth_real, (at - side) % LANES, 1), total)
            packed[group] = total

    pl.semaphore_wait(barrier, jnp.where(bottom, 3, 4))

    def send(source, target, slot, device, send_slot=None):
        return pltpu.make_async_remote_copy(
            src_ref=source,
            dst_ref=target,
            send_sem=send_sem.at[slot if send_slot is None else send_slot],
            recv_sem=recv_sem.at[slot],
            device_id=device,
            device_id_type=MESH,
        )

    def to_north_halo(source, depth_row, device, first_send):
        copies = [send(depth_row, depth_north, 0, device, first_send)]
        for chunk in range(chunks):
            part = pl.ds(chunk * per_chunk, per_chunk)
            slot = 1 + chunk
            copies.append(send(source.at[part], from_north.at[part], slot, device, first_send + slot))
        return copies

    base = 1 + chunks
    own_south = depth.at[pl.ds(0, 1)]
    own_north = depth.at[pl.ds(ROWS - 1, 1)]
    fold = to_north_halo(row_north, own_north, north, base + 4)
    down = to_north_halo(row_south, own_south, south, 0)
    upward = [
        send(own_north, depth_south, base, north),
        send(row_north, from_south, base + 1, north),
    ]
    across = [
        send(to_west, from_east, base + 2, west),
        send(to_east, from_west, base + 3, east),
    ]

    @pl.when(top)
    def _():
        for copy in fold:
            copy.start()

    for copy in across:
        copy.start()

    @pl.when(jnp.logical_not(top))
    def _():
        for copy in upward:
            copy.start()

    @pl.when(jnp.logical_not(bottom))
    def _():
        for copy in down:
            copy.start()

    @pl.when(bottom)
    def _():
        from_south[...] = jnp.zeros_like(from_south)
        depth_south[...] = jnp.zeros_like(depth_south)

    for copy in across:
        copy.wait_recv()

    @pl.when(jnp.logical_not(bottom))
    def _():
        for copy in upward:
            copy.wait_recv()

    spot = groups - 1
    spot_lane = (channels * LEVELS) % LANES
    part_level = lane % LEVELS

    def side_column(packed):
        first = packed[0]
        density = HALINE * pltpu.roll(first, LANES - LEVELS, 1) - THERMAL * first
        limit = packed[spot][:, spot_lane : spot_lane + 1]
        limit = jnp.broadcast_to(limit, shape).astype(jnp.int32)
        _, strat = vertical_pair(density, below(limit, part_level + 1), 1)
        return density, strat, limit

    west_density, west_strat, west_limit = side_column(from_west)
    east_density, east_strat, east_limit = side_column(from_east)

    south_density = HALINE * from_south[1] - THERMAL * from_south[0]
    south_limit = depth_south[...]
    row_level = row
    south_mask = below(jnp.broadcast_to(south_limit, shape), row_level + 1)
    _, south_strat = vertical_pair(south_density, south_mask, 0)

    density = [HALINE * field[1, k] - THERMAL * field[0, k] for k in range(LEVELS)]
    level_mask = [below(depth_here, k + 1) for k in range(LEVELS - 1)]
    strat_face = [(density[k + 1] - density[k]) * level_mask[k] for k in range(LEVELS - 1)]
    strat = [strat_face[0]]
    strat += [strat_face[k - 1] + strat_face[k] for k in range(1, LEVELS - 1)]
    strat += [strat_face[LEVELS - 2]]
    depth_west = jnp.minimum(depth_here, jnp.where(lane == 0, west_limit, pltpu.roll(depth_here, 1, 1)))
    depth_east = jnp.minimum(
        depth_here, jnp.where(lane == LANES - 1, east_limit, pltpu.roll(depth_here, LANES - 1, 1))
    )
    depth_down = jnp.minimum(
        depth_here,
        jnp.where(row == 0, jnp.broadcast_to(south_limit, shape), pltpu.roll(depth_here, 1, 0)),
    )
    inner_x = jnp.where(lane > 0, 1.0, 0.0)
    inner_y = jnp.where(row > 0, 1.0, 0.0)
    lower_rows = jnp.where(row < ROWS - 1, 1.0, 0.0)
    sum_x, sum_y, faces = [], [], []
    for k in range(LEVELS):
        mask_w, mask_e, mask_s = (below(limit, k) for limit in (depth_west, depth_east, depth_down))

        def from_side(edge, values, packed, shift):
            return jnp.where(lane == edge, pltpu.roll(packed, (edge - k) % LANES, 1), pltpu.roll(values, shift, 1))

        def from_below(values, compact):
            edge = jnp.broadcast_to(compact[k : k + 1], shape)
            return jnp.where(row == 0, edge, pltpu.roll(values, 1, 0))

        slope_w = slope_of(
            density[k] - from_side(0, density[k], west_density, 1),
            mask_w,
            strat[k] + from_side(0, strat[k], west_strat, 1),
        )
        slope_e = slope_of(
            from_side(LANES - 1, density[k], east_density, LANES - 1) - density[k],
            mask_e,
            strat[k] + from_side(LANES - 1, strat[k], east_strat, LANES - 1),
        )
        slope_s = slope_of(
            density[k] - from_below(density[k], south_density),
            mask_s,
            strat[k] + from_below(strat[k], south_strat),
        )
        slope_n = up_one(slope_s, 0) * lower_rows
        sum_x.append(slope_w + slope_e)
        sum_y.append(slope_s + slope_n)
        faces.append((mask_w, mask_e, mask_s, slope_w, slope_e, slope_s))

    zero = jnp.zeros(shape, jnp.float32)
    edges = [zero] * 6
    for k in range(LEVELS):
        mask_w, mask_e, mask_s, slope_w, slope_e, slope_s = faces[k]
        grad_w, flux_w = REDI_COEF * mask_w, SLOPE_FLUX * slope_w
        grad_e, flux_e = REDI_COEF * mask_e, SLOPE_FLUX * slope_e
        grad_s, flux_s = REDI_COEF * mask_s, SLOPE_FLUX * slope_s
        coef[0, k] = grad_w * inner_x
        coef[1, k] = flux_w * inner_x
        coef[2, k] = grad_s * inner_y
        coef[3, k] = flux_s * inner_y
        row_coef[0, pl.ds(k, 1)] = grad_s[0:1]
        row_coef[1, pl.ds(k, 1)] = flux_s[0:1]
        row_coef[3, pl.ds(k, 1)] = grad_s[ROWS - 1 : ROWS]
        row_coef[4, pl.ds(k, 1)] = slope_s[ROWS - 1 : ROWS]
        if k < LEVELS - 1:
            mean_x = 0.25 * (sum_x[k] + sum_x[k + 1])
            mean_y = 0.25 * (sum_y[k] + sum_y[k + 1])
            cross_x = CROSS * mean_x * level_mask[k]
            cross_y = CROSS * mean_y * level_mask[k]
            square = REDI_COEF * (mean_x * mean_x + mean_y * mean_y)
            coef[7, k] = level_mask[k]
        else:
            mean_x, cross_x, cross_y, square = zero, zero, zero, zero
            coef[7, k] = zero
        coef[4, k] = cross_x
        coef[5, k] = cross_y * lower_rows
        coef[6, k] = square * lower_rows
        row_coef[2, pl.ds(k, 1)] = cross_y[0:1]
        row_coef[5, pl.ds(k, 1)] = mean_x[ROWS - 1 : ROWS]
        news = (
            (grad_w, 0), (flux_w, 0), (cross_x, 0),
            (grad_e, LANES - 1), (flux_e, LANES - 1), (cross_x, LANES - 1),
        )
        edges = [
            jnp.where(part_level == k, jnp.broadcast_to(new[:, at : at + 1], shape), old)
            for (new, at), old in zip(news, edges)
        ]

    here_w = below(jnp.broadcast_to(depth_here[:, 0:1], shape), part_level + 1)
    here_e = below(jnp.broadcast_to(depth_here[:, LANES - 1 : LANES], shape), part_level + 1)
    there_w, there_e = below(west_limit, part_level + 1), below(east_limit, part_level + 1)
    for group in range(groups):
        own, other = to_west[group], from_west[group]
        grad = edges[0] * (own - other)
        pair = vertical_pair(own, here_w, 1)[1] + vertical_pair(other, there_w, 1)[1]
        vertical = edges[2] * (grad + up_one(grad, 1))
        edge_x[0, group] = vertical - pltpu.roll(vertical, 1, 1) - (grad + edges[1] * pair)
        own, other = to_east[group], from_east[group]
        grad = edges[3] * (other - own)
        pair = vertical_pair(own, here_e, 1)[1] + vertical_pair(other, there_e, 1)[1]
        vertical = edges[5] * (grad + up_one(grad, 1))
        edge_x[1, group] = vertical - pltpu.roll(vertical, 1, 1) + (grad + edges[4] * pair)

    own_south_limit = jnp.broadcast_to(depth_here[0:1], shape)
    own_south_mask = below(own_south_limit, row_level + 1)
    own_north_limit = jnp.broadcast_to(depth_here[ROWS - 1 : ROWS], shape)
    own_north_mask = below(own_north_limit, row_level + 1)

    def one_tracer(tracer, carry):
        values = [field[tracer, k] for k in range(LEVELS)]
        diff = [(values[k + 1] - values[k]) * coef[7, k] for k in range(LEVELS - 1)]
        pair = [diff[0]] + [diff[k - 1] + diff[k] for k in range(1, LEVELS - 1)] + [diff[LEVELS - 2]]
        group, slot = tracer // per_group, lax.rem(tracer, per_group)
        edge_w = pltpu.roll(edge_x[0, group], LANES - slot * LEVELS, 1)
        edge_e = pltpu.roll(edge_x[1, group], LANES - slot * LEVELS, 1)
        grads_x, grads_y, sides = [], [], []
        for k in range(LEVELS):
            grad_w = coef[0, k] * (values[k] - pltpu.roll(values[k], 1, 1))
            flux_w = grad_w + coef[1, k] * (pair[k] + pltpu.roll(pair[k], 1, 1))
            grad_s = coef[2, k] * (values[k] - pltpu.roll(values[k], 1, 0))
            flux_s = grad_s + coef[3, k] * (pair[k] + pltpu.roll(pair[k], 1, 0))
            grads_x.append(grad_w + up_one(grad_w, 1))
            grads_y.append(grad_s + up_one(grad_s, 0))
            side = jnp.where(lane == LANES - 1, pltpu.roll(edge_e, LANES - 1 - k, 1), zero)
            side = jnp.where(lane == 0, pltpu.roll(edge_w, (LANES - k) % LANES, 1), side)
            sides.append(values[k] + (up_one(flux_w, 1) - flux_w) + (up_one(flux_s, 0) - flux_s) + side)
        above = None
        for k in range(LEVELS):
            total = sides[k]
            if k < LEVELS - 1:
                vertical = (
                    coef[4, k] * (grads_x[k] + grads_x[k + 1])
                    + coef[5, k] * (grads_y[k] + grads_y[k + 1])
                    + coef[6, k] * diff[k]
                )
                total = total + vertical
            else:
                vertical = None
            if above is not None:
                total = total - above
            out[tracer, k] = total
            above = vertical
        own, other = row_south[tracer], from_south[tracer]
        grad = row_coef[0] * (own - other)
        both = vertical_pair(own, own_south_mask, 0)[1] + vertical_pair(other, south_mask, 0)[1]
        vertical = row_coef[2] * (grad + up_one(grad, 0))
        change = vertical - pltpu.roll(vertical, 1, 0) - (grad + row_coef[1] * both)
        out[tracer, :, 0, :] = out[tracer, :, 0, :] + change
        return carry

    lax.fori_loop(0, channels, one_tracer, 0)

    source_lane = jnp.where(top, LANES - 1 - lane, lane)

    def arranged(values):
        return jnp.take_along_axis(values, source_lane, axis=1, mode="promise_in_bounds")

    down[0].wait_recv()
    down[1].wait_recv()
    north_limit = arranged(jnp.broadcast_to(depth_north[...], shape))
    north_mask = below(north_limit, row_level + 1)
    face_mask = below(jnp.minimum(own_north_limit, north_limit), row_level)
    own_density = HALINE * row_north[1] - THERMAL * row_north[0]
    north_density = arranged(HALINE * from_north[1] - THERMAL * from_north[0])
    _, own_strat = vertical_pair(own_density, own_north_mask, 0)
    _, north_strat = vertical_pair(north_density, north_mask, 0)
    slope_n = slope_of(north_density - own_density, face_mask, own_strat + north_strat)
    sum_n = slope_n + row_coef[4]
    mean_n = 0.25 * (sum_n + up_one(sum_n, 0))
    mean_x = row_coef[5]
    cross_n = CROSS * mean_n * own_north_mask
    square_n = REDI_COEF * (mean_x * mean_x + mean_n * mean_n)
    grad_n, flux_n, grad_in = REDI_COEF * face_mask, SLOPE_FLUX * slope_n, row_coef[3]

    def north_face(tracer, carry):
        own, other = row_north[tracer], arranged(from_north[tracer])
        grad = grad_n * (other - own)
        diff, pair = vertical_pair(own, own_north_mask, 0)
        both = pair + vertical_pair(other, north_mask, 0)[1]
        grads = grad + grad_in * (own - row_inner[tracer])
        vertical = cross_n * (grads + up_one(grads, 0)) + square_n * diff
        change = vertical - pltpu.roll(vertical, 1, 0) + (grad + flux_n * both)
        out[tracer, :, ROWS - 1, :] = out[tracer, :, ROWS - 1, :] + change
        return carry

    for chunk in range(chunks):
        if chunk:
            down[1 + chunk].wait_recv()
        lax.fori_loop(chunk * per_chunk, (chunk + 1) * per_chunk, north_face, 0)

    for copy in across:
        copy.wait_send()

    @pl.when(top)
    def _():
        for copy in fold:
            copy.wait_send()

    @pl.when(jnp.logical_not(top))
    def _():
        for copy in upward:
            copy.wait_send()

    @pl.when(jnp.logical_not(bottom))
    def _():
        for copy in down:
            copy.wait_send()


def local(tracers, kmt):
    channels = tracers.shape[0]
    chunks = 4
    groups = -(-(channels * LEVELS + 1) // LANES)
    row_array = VMEM((channels, LEVELS, LANES), jnp.float32)
    packed = VMEM((groups, ROWS, LANES), jnp.float32)
    depth_row = VMEM((1, LANES), jnp.int32)
    anywhere = pl.BlockSpec(memory_space=pl.ANY)
    return pl.pallas_call(
        functools.partial(kernel, channels, chunks),
        out_shape=jax.ShapeDtypeStruct(tracers.shape, jnp.float32),
        in_specs=[anywhere, anywhere],
        out_specs=pl.BlockSpec(memory_space=VMEM),
        scratch_shapes=[
            VMEM(tracers.shape, jnp.float32),
            row_array, row_array, row_array, VMEM((ROWS, LANES), jnp.int32),
            row_array, row_array, depth_row, depth_row,
            packed, packed, packed, packed,
            VMEM((8, LEVELS, ROWS, LANES), jnp.float32),
            VMEM((2, groups, ROWS, LANES), jnp.float32),
            VMEM((6, LEVELS, LANES), jnp.float32),
            pltpu.SemaphoreType.DMA((5,)),
            pltpu.SemaphoreType.DMA((2 * chunks + 6,)),
            pltpu.SemaphoreType.DMA((chunks + 5,)),
        ],
        compiler_params=pltpu.CompilerParams(collective_id=0, has_side_effects=True),
        name="tracer_step",
    )(tracers, kmt)


def solution(mesh):
    return jax.shard_map(
        local,
        mesh=mesh,
        in_specs=(P(None, None, "lat", "lon"), P("lat", "lon")),
        out_specs=P(None, None, "lat", "lon"),
        check_vma=False,
    )
```

```python
import functools

import jax
import jax.numpy as jnp
from jax import lax
from jax.experimental import pallas as pl
from jax.experimental.pallas import tpu as pltpu
from jax.sharding import PartitionSpec as P

THERMAL = 0.2
HALINE = 0.8
REDI_COEF = 0.1
SKEW_COEF = 0.05
SLOPE_MAX = 0.6
SLOPE_WIDTH = 0.2
SLOPE_FLUX = (REDI_COEF - SKEW_COEF) * 0.25
CROSS = (REDI_COEF + SKEW_COEF) * 0.25 / REDI_COEF

ROWS = 8
LANES = 128
LEVELS = 8
MESH = pl.DeviceIdType.MESH
VMEM = pltpu.VMEM


def taper(slope):
    return slope * 0.5 * (1.0 + jnp.tanh((SLOPE_MAX - jnp.abs(slope)) / SLOPE_WIDTH))


def slope_of(step, mask, strat_twice):
    return taper(step * mask / jnp.maximum(0.25 * strat_twice, 1.0))


def below(limit, level):
    return jnp.where(level < limit, 1.0, 0.0)


def vertical_pair(values, mask, axis):
    size = values.shape[axis]
    diff = (pltpu.roll(values, size - 1, axis) - values) * mask
    return diff, diff + pltpu.roll(diff, 1, axis)


def up_one(values, axis):
    return pltpu.roll(values, values.shape[axis] - 1, axis)


def kernel(
    channels, chunks, tracers, kmt, out,
    field, row_south, row_inner, row_north, depth,
    from_south, from_north, depth_south, depth_north,
    sides, from_west, from_east,
    coef, part, edge, row_coef,
    load_sem, send_sem, recv_sem,
):
    lon, lat = lax.axis_index("lon"), lax.axis_index("lat")
    blocks, bands = lax.axis_size("lon"), lax.axis_size("lat")
    top, bottom = lat == bands - 1, lat == 0
    west = (lax.rem(lon + blocks - 1, blocks), lat)
    east = (lax.rem(lon + 1, blocks), lat)
    north = (jnp.where(top, blocks - 1 - lon, lon), jnp.where(top, lat, lat + 1))
    south = (lon, jnp.maximum(lat - 1, 0))
    per_chunk = channels // chunks

    barrier = pltpu.get_barrier_semaphore()
    for other in (north, west, east):
        pl.semaphore_signal(barrier, inc=1, device_id=other, device_id_type=MESH)

    @pl.when(jnp.logical_not(bottom))
    def _():
        pl.semaphore_signal(barrier, inc=1, device_id=south, device_id_type=MESH)

    loads = [
        pltpu.make_async_copy(kmt, depth, load_sem.at[2]),
        pltpu.make_async_copy(tracers, field, load_sem.at[1]),
        pltpu.make_async_copy(tracers.at[:, :, ROWS - 1, :], row_north, load_sem.at[0]),
        pltpu.make_async_copy(tracers.at[:, :, 0, :], row_south, load_sem.at[3]),
        pltpu.make_async_copy(tracers.at[:, :, ROWS - 2, :], row_inner, load_sem.at[4]),
    ]
    for load in loads:
        load.start()
    for load in loads:
        load.wait()

    shape = (ROWS, LANES)
    lane = lax.broadcasted_iota(jnp.int32, shape, 1)
    row = lax.broadcasted_iota(jnp.int32, shape, 0)
    zero = jnp.zeros(shape, jnp.float32)
    depth_here = depth[...]

    def right(values, count=1):
        return pltpu.roll(values, count % LANES, 1)

    def wide(values):
        return jnp.broadcast_to(values, shape)

    density = [HALINE * field[1, k] - THERMAL * field[0, k] for k in range(LEVELS)]
    level_mask = [below(depth_here, k + 1) for k in range(LEVELS - 1)]
    strat_face = [(density[k + 1] - density[k]) * level_mask[k] for k in range(LEVELS - 1)]
    strat = [strat_face[0]]
    strat += [strat_face[k - 1] + strat_face[k] for k in range(1, LEVELS - 1)]
    strat += [strat_face[LEVELS - 2]]
    depth_left = jnp.minimum(depth_here, jnp.where(lane == 0, 0, right(depth_here)))
    depth_right = jnp.minimum(depth_here, jnp.where(lane == LANES - 1, 0, right(depth_here, -1)))
    depth_down = jnp.minimum(depth_here, jnp.where(row == 0, 0, pltpu.roll(depth_here, 1, 0)))
    for k in range(LEVELS):
        mask_w, mask_e, mask_s = (below(limit, k) for limit in (depth_left, depth_right, depth_down))
        slope_w = slope_of(density[k] - right(density[k]), mask_w, strat[k] + right(strat[k]))
        slope_e = slope_of(right(density[k], -1) - density[k], mask_e, strat[k] + right(strat[k], -1))
        slope_s = slope_of(
            density[k] - pltpu.roll(density[k], 1, 0), mask_s, strat[k] + pltpu.roll(strat[k], 1, 0)
        )
        coef[0, k] = REDI_COEF * mask_w
        coef[1, k] = REDI_COEF * mask_e
        coef[2, k] = REDI_COEF * mask_s
        coef[3, k] = SLOPE_FLUX * slope_w
        coef[4, k] = SLOPE_FLUX * slope_e
        coef[5, k] = SLOPE_FLUX * slope_s
        coef[6, k] = level_mask[k] if k < LEVELS - 1 else zero
        coef[7, k] = slope_w + slope_e
        coef[8, k] = slope_s + up_one(slope_s, 0)
        row_coef[0, pl.ds(k, 1)] = slope_s[ROWS - 1 : ROWS]
        row_coef[1, pl.ds(k, 1)] = mask_s[ROWS - 1 : ROWS]

    pair_id = lax.rem(lane + 1, LANES) // 2
    per_group = LANES // 2 // LEVELS
    groups = channels // per_group
    sides[groups] = depth_here.astype(jnp.float32)

    def one_group(group, carry):
        packed = zero
        for slot in range(per_group):
            tracer = group * per_group + slot
            values = [field[tracer, k] for k in range(LEVELS)]
            for k in range(LEVELS):
                at = slot * LEVELS + k
                packed = jnp.where(pair_id == at, right(values[k], 2 * at), packed)
            diff = [(values[k + 1] - values[k]) * coef[6, k] for k in range(LEVELS - 1)]
            pair = [diff[0]] + [diff[k - 1] + diff[k] for k in range(1, LEVELS - 1)] + [diff[LEVELS - 2]]
            grad_x, grad_y = [], []
            for k in range(LEVELS):
                here, both = values[k], pair[k]
                grad_w = coef[0, k] * (here - right(here))
                grad_e = coef[1, k] * (right(here, -1) - here)
                grad_s = coef[2, k] * (here - pltpu.roll(here, 1, 0))
                flux_w = grad_w + coef[3, k] * (both + right(both))
                flux_e = grad_e + coef[4, k] * (both + right(both, -1))
                flux_s = grad_s + coef[5, k] * (both + pltpu.roll(both, 1, 0))
                grad_x.append(grad_w + grad_e)
                grad_y.append(grad_s + up_one(grad_s, 0))
                part[0, tracer, k] = here + (flux_e - flux_w) + (up_one(flux_s, 0) - flux_s)
            for k in range(LEVELS - 1):
                part[1, tracer, k] = grad_x[k] + grad_x[k + 1]
                part[2, tracer, k] = grad_y[k] + grad_y[k + 1]
                part[3, tracer, k] = diff[k]
        sides[group] = packed
        return carry

    lax.fori_loop(0, groups, one_group, 0)

    pl.semaphore_wait(barrier, jnp.where(bottom, 3, 4))

    def send(source, target, slot, device, send_slot=None):
        return pltpu.make_async_remote_copy(
            src_ref=source,
            dst_ref=target,
            send_sem=send_sem.at[slot if send_slot is None else send_slot],
            recv_sem=recv_sem.at[slot],
            device_id=device,
            device_id_type=MESH,
        )

    def to_north_halo(source, depth_row, device, first_send):
        copies = [send(depth_row, depth_north, 0, device, first_send)]
        for chunk in range(chunks):
            span = pl.ds(chunk * per_chunk, per_chunk)
            slot = 1 + chunk
            copies.append(send(source.at[span], from_north.at[span], slot, device, first_send + slot))
        return copies

    base = 1 + chunks
    own_south = depth.at[pl.ds(0, 1)]
    own_north = depth.at[pl.ds(ROWS - 1, 1)]
    fold = to_north_halo(row_north, own_north, north, base + 4)
    down = to_north_halo(row_south, own_south, south, 0)
    upward = [
        send(own_north, depth_south, base, north),
        send(row_north, from_south, base + 1, north),
    ]
    across = [
        send(sides, from_east, base + 2, west),
        send(sides, from_west, base + 3, east),
    ]

    @pl.when(top)
    def _():
        for copy in fold:
            copy.start()

    for copy in across:
        copy.start()

    @pl.when(jnp.logical_not(top))
    def _():
        for copy in upward:
            copy.start()

    @pl.when(jnp.logical_not(bottom))
    def _():
        for copy in down:
            copy.start()

    @pl.when(bottom)
    def _():
        from_south[...] = jnp.zeros_like(from_south)
        depth_south[...] = jnp.zeros_like(depth_south)

    for copy in across:
        copy.wait_recv()

    @pl.when(jnp.logical_not(bottom))
    def _():
        for copy in upward:
            copy.wait_recv()

    even = lax.rem(lane, 2) == 0
    at_edge = jnp.logical_or(lane == 0, lane == LANES - 1)
    side_level = lax.rem(pair_id, LEVELS)

    def beside(group):
        return jnp.where(even, right(from_west[group]), right(from_east[group], -1))

    def side_pair(values, mask):
        diff = (right(values, -2) - values) * mask
        return diff + right(diff, 2)

    west_limit = wide(from_west[groups][:, LANES - 1 : LANES]).astype(jnp.int32)
    east_limit = wide(from_east[groups][:, 0:1]).astype(jnp.int32)
    there_limit = jnp.where(even, west_limit, east_limit)
    here_limit = jnp.where(even, wide(depth_here[:, 0:1]), wide(depth_here[:, LANES - 1 : LANES]))
    there_mask, here_mask = below(there_limit, side_level + 1), below(here_limit, side_level + 1)
    side_mask = below(jnp.minimum(there_limit, here_limit), side_level)
    first_there, first_here = beside(0), sides[0]
    density_there = HALINE * right(first_there, -2 * LEVELS) - THERMAL * first_there
    density_here = HALINE * right(first_here, -2 * LEVELS) - THERMAL * first_here
    side_sign = jnp.where(even, -1.0, 1.0)
    side_slope = slope_of(
        side_sign * (density_there - density_here),
        side_mask,
        side_pair(density_there, there_mask) + side_pair(density_here, here_mask),
    )

    south_limit = wide(depth_south[...])
    south_mask = below(south_limit, row + 1)
    low_limit = wide(depth_here[0:1])
    low_mask = below(low_limit, row + 1)
    south_face = below(jnp.minimum(south_limit, low_limit), row)
    density_south = HALINE * from_south[1] - THERMAL * from_south[0]
    density_low = HALINE * row_south[1] - THERMAL * row_south[0]
    slope_south = slope_of(
        density_low - density_south,
        south_face,
        vertical_pair(density_south, south_mask, 0)[1] + vertical_pair(density_low, low_mask, 0)[1],
    )

    sum_x, sum_y = [], []
    for k in range(LEVELS):
        outer = jnp.where(at_edge, right(side_slope, -2 * k), 0.0)
        sum_x.append(coef[7, k] + outer)
        sum_y.append(coef[8, k] + jnp.where(row == 0, wide(slope_south[k : k + 1]), 0.0))
    lower_rows = jnp.where(row < ROWS - 1, 1.0, 0.0)
    side_cross = zero
    row_coef[2] = zero
    row_coef[3] = zero
    for k in range(LEVELS - 1):
        mean_x = 0.25 * (sum_x[k] + sum_x[k + 1])
        mean_y = 0.25 * (sum_y[k] + sum_y[k + 1])
        cross_x = CROSS * mean_x * coef[6, k]
        cross_y = CROSS * mean_y * coef[6, k]
        coef[0, k] = cross_x
        coef[1, k] = cross_y * lower_rows
        coef[2, k] = REDI_COEF * (mean_x * mean_x + mean_y * mean_y) * lower_rows
        row_coef[2, pl.ds(k, 1)] = cross_y[0:1]
        row_coef[3, pl.ds(k, 1)] = mean_x[ROWS - 1 : ROWS]
        ends = jnp.where(even, wide(cross_x[:, 0:1]), wide(cross_x[:, LANES - 1 : LANES]))
        side_cross = jnp.where(side_level == k, ends, side_cross)
    side_cross = side_cross * side_sign
    side_flux = jnp.where(pair_id < LEVELS, side_slope * side_sign * SLOPE_FLUX, 0.0)
    shift = 2 * LEVELS
    while shift < LANES:
        side_flux = side_flux + right(side_flux, shift)
        shift *= 2
    side_grad = REDI_COEF * side_mask

    for group in range(groups):
        own, other = sides[group], beside(group)
        grad = side_grad * (other - own)
        pair = side_pair(own, here_mask) + side_pair(other, there_mask)
        vertical = side_cross * (grad + right(grad, -2))
        edge[group] = vertical - right(vertical, 2) + grad + side_flux * pair

    def finish_group(group, carry):
        added = edge[group]
        for slot in range(per_group):
            tracer = group * per_group + slot
            above = None
            for k in range(LEVELS):
                at = slot * LEVELS + k
                total = part[0, tracer, k] + jnp.where(at_edge, right(added, -2 * at), 0.0)
                if k < LEVELS - 1:
                    vertical = (
                        coef[0, k] * part[1, tracer, k]
                        + coef[1, k] * part[2, tracer, k]
                        + coef[2, k] * part[3, tracer, k]
                    )
                    total = total + vertical
                if k > 0:
                    total = total - above
                above = vertical
                out[tracer, k] = total
        return carry

    lax.fori_loop(0, groups, finish_group, 0)

    grad_low, flux_low, cross_low = REDI_COEF * south_face, SLOPE_FLUX * slope_south, row_coef[2]

    def south_face_group(group, carry):
        for slot in range(per_group):
            tracer = group * per_group + slot
            own, other = row_south[tracer], from_south[tracer]
            grad = grad_low * (own - other)
            both = vertical_pair(own, low_mask, 0)[1] + vertical_pair(other, south_mask, 0)[1]
            vertical = cross_low * (grad + up_one(grad, 0))
            change = vertical - pltpu.roll(vertical, 1, 0) - (grad + flux_low * both)
            out[tracer, :, 0, :] = out[tracer, :, 0, :] + change
        return carry

    lax.fori_loop(0, groups, south_face_group, 0)

    source_lane = jnp.where(top, LANES - 1 - lane, lane)

    def arranged(values):
        return jnp.take_along_axis(values, source_lane, axis=1, mode="promise_in_bounds")

    high_limit = wide(depth_here[ROWS - 1 : ROWS])
    high_mask = below(high_limit, row + 1)
    density_high = HALINE * row_north[1] - THERMAL * row_north[0]
    strat_high = vertical_pair(density_high, high_mask, 0)[1]
    mean_x = row_coef[3]
    grad_in = REDI_COEF * row_coef[1]

    down[0].wait_recv()
    down[1].wait_recv()
    north_limit = arranged(wide(depth_north[...]))
    north_mask = below(north_limit, row + 1)
    north_face = below(jnp.minimum(high_limit, north_limit), row)
    density_north = arranged(HALINE * from_north[1] - THERMAL * from_north[0])
    strat_north = vertical_pair(density_north, north_mask, 0)[1]
    slope_north = slope_of(density_north - density_high, north_face, strat_high + strat_north)
    sum_n = slope_north + row_coef[0]
    mean_n = 0.25 * (sum_n + up_one(sum_n, 0))
    cross_n = CROSS * mean_n * high_mask
    square_n = REDI_COEF * (mean_x * mean_x + mean_n * mean_n)
    grad_n, flux_n = REDI_COEF * north_face, SLOPE_FLUX * slope_north

    def north_face_of(tracer):
        own, other = row_north[tracer], arranged(from_north[tracer])
        grad = grad_n * (other - own)
        diff, pair = vertical_pair(own, high_mask, 0)
        both = pair + vertical_pair(other, north_mask, 0)[1]
        grads = grad + grad_in * (own - row_inner[tracer])
        vertical = cross_n * (grads + up_one(grads, 0)) + square_n * diff
        change = vertical - pltpu.roll(vertical, 1, 0) + (grad + flux_n * both)
        out[tracer, :, ROWS - 1, :] = out[tracer, :, ROWS - 1, :] + change

    for chunk in range(chunks):
        if chunk:
            down[1 + chunk].wait_recv()
        for tracer in range(chunk * per_chunk, (chunk + 1) * per_chunk):
            north_face_of(tracer)

    for copy in across:
        copy.wait_send()

    @pl.when(top)
    def _():
        for copy in fold:
            copy.wait_send()

    @pl.when(jnp.logical_not(top))
    def _():
        for copy in upward:
            copy.wait_send()

    @pl.when(jnp.logical_not(bottom))
    def _():
        for copy in down:
            copy.wait_send()


def local(tracers, kmt):
    channels = tracers.shape[0]
    chunks = 4
    groups = channels * LEVELS * 2 // LANES
    row_array = VMEM((channels, LEVELS, LANES), jnp.float32)
    packed = VMEM((groups + 1, ROWS, LANES), jnp.float32)
    depth_row = VMEM((1, LANES), jnp.int32)
    anywhere = pl.BlockSpec(memory_space=pl.ANY)
    return pl.pallas_call(
        functools.partial(kernel, channels, chunks),
        out_shape=jax.ShapeDtypeStruct(tracers.shape, jnp.float32),
        in_specs=[anywhere, anywhere],
        out_specs=pl.BlockSpec(memory_space=VMEM),
        scratch_shapes=[
            VMEM(tracers.shape, jnp.float32),
            row_array, row_array, row_array, VMEM((ROWS, LANES), jnp.int32),
            row_array, row_array, depth_row, depth_row,
            packed, packed, packed,
            VMEM((9, LEVELS, ROWS, LANES), jnp.float32),
            VMEM((4,) + tracers.shape, jnp.float32),
            VMEM((groups, ROWS, LANES), jnp.float32),
            VMEM((4, LEVELS, LANES), jnp.float32),
            pltpu.SemaphoreType.DMA((5,)),
            pltpu.SemaphoreType.DMA((2 * chunks + 6,)),
            pltpu.SemaphoreType.DMA((chunks + 5,)),
        ],
        compiler_params=pltpu.CompilerParams(collective_id=0, has_side_effects=True),
        name="tracer_step",
    )(tracers, kmt)


def solution(mesh):
    return jax.shard_map(
        local,
        mesh=mesh,
        in_specs=(P(None, None, "lat", "lon"), P("lat", "lon")),
        out_specs=P(None, None, "lat", "lon"),
        check_vma=False,
    )
```

```python
import functools

import jax
import jax.numpy as jnp
from jax import lax
from jax.experimental import pallas as pl
from jax.experimental.pallas import tpu as pltpu
from jax.sharding import PartitionSpec as P

THERMAL = 0.2
HALINE = 0.8
REDI_COEF = 0.1
SKEW_COEF = 0.05
SLOPE_MAX = 0.6
SLOPE_WIDTH = 0.2
SLOPE_FLUX = (REDI_COEF - SKEW_COEF) * 0.25
CROSS = (REDI_COEF + SKEW_COEF) * 0.25 / REDI_COEF

ROWS = 8
LANES = 128
LEVELS = 8
MESH = pl.DeviceIdType.MESH
VMEM = pltpu.VMEM


def taper(slope):
    return slope * 0.5 * (1.0 + jnp.tanh((SLOPE_MAX - jnp.abs(slope)) / SLOPE_WIDTH))


def slope_of(step, mask, strat_twice):
    return taper(step * mask / jnp.maximum(0.25 * strat_twice, 1.0))


def below(limit, level):
    return jnp.where(level < limit, 1.0, 0.0)


def vertical_pair(values, mask, axis):
    size = values.shape[axis]
    diff = (pltpu.roll(values, size - 1, axis) - values) * mask
    return diff, diff + pltpu.roll(diff, 1, axis)


def up_one(values, axis):
    return pltpu.roll(values, values.shape[axis] - 1, axis)


def kernel(
    channels, chunks, early, tracers, kmt, out,
    field, depth, from_south, from_north, depth_south, depth_north,
    sides, from_west, from_east,
    main, cross_x, coef, inner, edge, row_coef,
    load_sem, send_sem, recv_sem,
):
    lon, lat = lax.axis_index("lon"), lax.axis_index("lat")
    blocks, bands = lax.axis_size("lon"), lax.axis_size("lat")
    top, bottom = lat == bands - 1, lat == 0
    west = (lax.rem(lon + blocks - 1, blocks), lat)
    east = (lax.rem(lon + 1, blocks), lat)
    north = (jnp.where(top, blocks - 1 - lon, lon), jnp.where(top, lat, lat + 1))
    south = (lon, jnp.maximum(lat - 1, 0))
    per_chunk = channels // chunks
    per_group = LANES // 2 // LEVELS
    groups = channels // per_group

    barrier = pltpu.get_barrier_semaphore()
    for other in (north, west, east):
        pl.semaphore_signal(barrier, inc=1, device_id=other, device_id_type=MESH)

    @pl.when(jnp.logical_not(bottom))
    def _():
        pl.semaphore_signal(barrier, inc=1, device_id=south, device_id_type=MESH)

    loads = [
        pltpu.make_async_copy(kmt, depth, load_sem.at[0]),
        pltpu.make_async_copy(tracers, field, load_sem.at[1]),
    ]
    for load in loads:
        load.start()

    def send(source, target, slot, device, send_slot=None):
        return pltpu.make_async_remote_copy(
            src_ref=source,
            dst_ref=target,
            send_sem=send_sem.at[slot if send_slot is None else send_slot],
            recv_sem=recv_sem.at[slot],
            device_id=device,
            device_id_type=MESH,
        )

    def to_north_halo(own_row, device, first_send):
        copies = [send(kmt.at[pl.ds(own_row, 1)], depth_north, 0, device, first_send)]
        for chunk in range(chunks):
            span = pl.ds(chunk * per_chunk, per_chunk)
            slot = 1 + chunk
            source = tracers.at[span, :, own_row, :]
            copies.append(send(source, from_north.at[span], slot, device, first_send + slot))
        return copies

    base = 1 + chunks
    fold = to_north_halo(ROWS - 1, north, base + 4)
    down = to_north_halo(0, south, 0)
    upward = [
        send(kmt.at[pl.ds(ROWS - 1, 1)], depth_south, base, north),
        send(tracers.at[:, :, ROWS - 1, :], from_south, base + 1, north),
    ]
    across = [
        send(sides, from_east, base + 2, west),
        send(sides, from_west, base + 3, east),
    ]

    pl.semaphore_wait(barrier, jnp.where(bottom, 3, 4))

    @pl.when(jnp.logical_not(bottom))
    def _():
        for copy in down:
            copy.start()

    @pl.when(top)
    def _():
        for copy in fold[:early]:
            copy.start()

    @pl.when(jnp.logical_not(top))
    def _():
        for copy in upward:
            copy.start()

    for load in loads:
        load.wait()

    shape = (ROWS, LANES)
    lane = lax.broadcasted_iota(jnp.int32, shape, 1)
    row = lax.broadcasted_iota(jnp.int32, shape, 0)
    zero = jnp.zeros(shape, jnp.float32)
    depth_here = depth[...]

    def right(values, count=1):
        return pltpu.roll(values, count % LANES, 1)

    def wide(values):
        return jnp.broadcast_to(values, shape)

    pair_id = lax.rem(lane + 1, LANES) // 2
    sides[groups] = depth_here.astype(jnp.float32)
    for group in range(groups):
        packed = zero
        for at in range(LANES // 2):
            tracer, k = group * per_group + at // LEVELS, at % LEVELS
            packed = jnp.where(pair_id == at, right(field[tracer, k], 2 * at), packed)
        sides[group] = packed

    for copy in across:
        copy.start()

    @pl.when(top)
    def _():
        for copy in fold[early:]:
            copy.start()

    @pl.when(bottom)
    def _():
        from_south[...] = jnp.zeros_like(from_south)
        depth_south[...] = jnp.zeros_like(depth_south)

    density = [HALINE * field[1, k] - THERMAL * field[0, k] for k in range(LEVELS)]
    level_mask = [below(depth_here, k + 1) for k in range(LEVELS - 1)]
    strat_face = [(density[k + 1] - density[k]) * level_mask[k] for k in range(LEVELS - 1)]
    strat = [strat_face[0]]
    strat += [strat_face[k - 1] + strat_face[k] for k in range(1, LEVELS - 1)]
    strat += [strat_face[LEVELS - 2]]
    depth_left = jnp.minimum(depth_here, jnp.where(lane == 0, 0, right(depth_here)))
    depth_right = jnp.minimum(depth_here, jnp.where(lane == LANES - 1, 0, right(depth_here, -1)))
    depth_down = jnp.minimum(depth_here, jnp.where(row == 0, 0, pltpu.roll(depth_here, 1, 0)))
    at_edge = jnp.logical_or(lane == 0, lane == LANES - 1)
    inner_lanes = jnp.where(at_edge, 0.0, 1.0)
    inner_rows = jnp.where(jnp.logical_or(row == 0, row == ROWS - 1), 0.0, 1.0)
    sum_x, sum_y = [], []
    inner_slope = zero
    for k in range(LEVELS):
        mask_w, mask_e, mask_s = (below(limit, k) for limit in (depth_left, depth_right, depth_down))
        slope_w = slope_of(density[k] - right(density[k]), mask_w, strat[k] + right(strat[k]))
        slope_e = slope_of(right(density[k], -1) - density[k], mask_e, strat[k] + right(strat[k], -1))
        slope_s = slope_of(
            density[k] - pltpu.roll(density[k], 1, 0), mask_s, strat[k] + pltpu.roll(strat[k], 1, 0)
        )
        coef[0, k] = REDI_COEF * mask_w
        coef[1, k] = REDI_COEF * mask_e
        coef[2, k] = REDI_COEF * mask_s
        coef[3, k] = SLOPE_FLUX * slope_w
        coef[4, k] = SLOPE_FLUX * slope_e
        coef[5, k] = SLOPE_FLUX * slope_s
        coef[6, k] = level_mask[k] if k < LEVELS - 1 else zero
        sum_x.append(slope_w + slope_e)
        sum_y.append(slope_s + up_one(slope_s, 0))
        inner_slope = jnp.where(pair_id == k, right(sum_x[k], 2 * k), inner_slope)
        row_coef[0, pl.ds(k, 1)] = slope_s[1:2]
        row_coef[1, pl.ds(k, 1)] = REDI_COEF * mask_s[1:2]
        row_coef[2, pl.ds(k, 1)] = slope_s[ROWS - 1 : ROWS]
        row_coef[3, pl.ds(k, 1)] = REDI_COEF * mask_s[ROWS - 1 : ROWS]
    for k in range(LEVELS - 1):
        mean_x = 0.25 * (sum_x[k] + sum_x[k + 1]) * inner_lanes
        mean_y = 0.25 * (sum_y[k] + sum_y[k + 1]) * inner_rows
        coef[7, k] = CROSS * mean_x * level_mask[k]
        coef[8, k] = CROSS * mean_y * level_mask[k]
        coef[9, k] = REDI_COEF * (mean_x * mean_x + mean_y * mean_y)

    def one_group(group, carry):
        for slot in range(per_group):
            tracer = group * per_group + slot
            values = [field[tracer, k] for k in range(LEVELS)]
            diff = [(values[k + 1] - values[k]) * coef[6, k] for k in range(LEVELS - 1)]
            pair = [diff[0]] + [diff[k - 1] + diff[k] for k in range(1, LEVELS - 1)] + [diff[LEVELS - 2]]
            grad_x, grad_y, total = [], [], []
            for k in range(LEVELS):
                here, both = values[k], pair[k]
                grad_w = coef[0, k] * (here - right(here))
                grad_e = coef[1, k] * (right(here, -1) - here)
                grad_s = coef[2, k] * (here - pltpu.roll(here, 1, 0))
                flux_w = grad_w + coef[3, k] * (both + right(both))
                flux_e = grad_e + coef[4, k] * (both + right(both, -1))
                flux_s = grad_s + coef[5, k] * (both + pltpu.roll(both, 1, 0))
                grad_x.append(grad_w + grad_e)
                grad_y.append(grad_s + up_one(grad_s, 0))
                total.append(here + (flux_e - flux_w) + (up_one(flux_s, 0) - flux_s))
            above = None
            for k in range(LEVELS):
                added = total[k] if above is None else total[k] - above
                if k < LEVELS - 1:
                    both_x, both_y = grad_x[k] + grad_x[k + 1], grad_y[k] + grad_y[k + 1]
                    cross_x[tracer, k] = both_x
                    above = coef[7, k] * both_x + coef[8, k] * both_y + coef[9, k] * diff[k]
                    added = added + above
                main[tracer, k] = added
        return carry

    lax.fori_loop(0, groups, one_group, 0)

    for group in range(groups):
        packed = zero
        for at in range(LANES // 2):
            tracer, k = group * per_group + at // LEVELS, at % LEVELS
            if k < LEVELS - 1:
                packed = jnp.where(pair_id == at, right(cross_x[tracer, k], 2 * at), packed)
        inner[group] = packed

    source_lane = jnp.where(top, LANES - 1 - lane, lane)

    def mirrored(values):
        return jnp.take_along_axis(values, source_lane, axis=1, mode="promise_in_bounds")

    def row_terms(at, beyond, depth_beyond, arranged, first):
        sign = 1.0 if at else -1.0
        beside_row = at - 1 if at else 1
        limit = wide(depth_here[at : at + 1])
        mask = below(limit, row + 1)
        limit_beyond = arranged(wide(depth_beyond[...]))
        mask_beyond = below(limit_beyond, row + 1)
        face = below(jnp.minimum(limit, limit_beyond), row)
        density_row = HALINE * field[1, :, at, :] - THERMAL * field[0, :, at, :]
        density_beyond = arranged(HALINE * beyond[1] - THERMAL * beyond[0])
        slope = slope_of(
            sign * (density_beyond - density_row),
            face,
            vertical_pair(density_row, mask, 0)[1] + vertical_pair(density_beyond, mask_beyond, 0)[1],
        )
        sums = slope + row_coef[first]
        mean = 0.25 * (sums + up_one(sums, 0))
        cross, square = CROSS * mean * mask, REDI_COEF * mean * mean
        grad_face, flux_face, grad_in = REDI_COEF * face, sign * SLOPE_FLUX * slope, row_coef[first + 1]

        def add(tracer, result):
            own, other = field[tracer, :, at, :], arranged(beyond[tracer])
            step = grad_face * (other - own)
            diff, pair = vertical_pair(own, mask, 0)
            both = pair + vertical_pair(other, mask_beyond, 0)[1]
            grads = sign * (step + grad_in * (own - field[tracer, :, beside_row, :]))
            vertical = cross * (grads + up_one(grads, 0)) + square * diff
            change = vertical - pltpu.roll(vertical, 1, 0) + (step + flux_face * both)
            result[tracer, :, at, :] = result[tracer, :, at, :] + change

        return add

    @pl.when(jnp.logical_not(bottom))
    def _():
        for copy in upward:
            copy.wait_recv()

    add_south = row_terms(0, from_south, depth_south, lambda values: values, 0)
    for tracer in range(channels):
        add_south(tracer, main)

    def north_face(result):
        for copy in down[:2]:
            copy.wait_recv()
        add_north = row_terms(ROWS - 1, from_north, depth_north, mirrored, 2)
        for chunk in range(chunks):
            if chunk:
                down[1 + chunk].wait_recv()
            for tracer in range(chunk * per_chunk, (chunk + 1) * per_chunk):
                add_north(tracer, result)

    pl.when(jnp.logical_not(top))(functools.partial(north_face, main))

    even = lax.rem(lane, 2) == 0
    side_level = lax.rem(pair_id, LEVELS)
    side_sign = jnp.where(even, -1.0, 1.0)
    span = 2 * LEVELS

    def beside(group, shift=0):
        return jnp.where(even, right(from_west[group], 1 - shift), right(from_east[group], -1 - shift))

    def side_pair(values, mask):
        diff = (right(values, -2) - values) * mask
        return diff, diff + right(diff, 2)

    def every_tracer(values):
        values = jnp.where(pair_id < LEVELS, values, 0.0)
        total = values
        for shift in range(span, LANES, span):
            total = total + right(values, shift)
        return total

    here_limit = jnp.where(even, wide(depth_here[:, 0:1]), wide(depth_here[:, LANES - 1 : LANES]))
    here_mask = below(here_limit, side_level + 1)
    density_side = HALINE * right(sides[0], -span) - THERMAL * sides[0]
    strat_side = side_pair(density_side, here_mask)[1]

    for copy in across:
        copy.wait_recv()

    west_limit = wide(from_west[groups][:, LANES - 1 : LANES]).astype(jnp.int32)
    east_limit = wide(from_east[groups][:, 0:1]).astype(jnp.int32)
    there_limit = jnp.where(even, west_limit, east_limit)
    there_mask = below(there_limit, side_level + 1)
    side_mask = below(jnp.minimum(there_limit, here_limit), side_level)
    density_there = HALINE * beside(0, span) - THERMAL * beside(0)
    side_slope = slope_of(
        side_sign * (density_there - density_side),
        side_mask,
        strat_side + side_pair(density_there, there_mask)[1],
    )
    sums = side_slope + inner_slope
    mean = 0.25 * (sums + right(sums, -2))
    side_flux = every_tracer(SLOPE_FLUX * side_sign * side_slope)
    side_mean = every_tracer(mean)
    side_cross = CROSS * side_mean * here_mask
    side_square = REDI_COEF * side_mean * side_mean
    side_grad = REDI_COEF * side_mask
    for group in range(groups):
        own, other = sides[group], beside(group)
        step = side_grad * (other - own)
        diff, pair = side_pair(own, here_mask)
        grads = inner[group] + side_sign * (step + right(step, -2))
        vertical = side_cross * grads + side_square * diff
        change = vertical - right(vertical, 2) + step + side_flux * (pair + side_pair(other, there_mask)[1])
        edge[group] = change
    for group in range(groups):
        change = edge[group]
        for at in range(LANES // 2):
            tracer, k = group * per_group + at // LEVELS, at % LEVELS
            out[tracer, k] = main[tracer, k] + jnp.where(at_edge, right(change, -2 * at), 0.0)

    pl.when(top)(functools.partial(north_face, out))

    for copy in across:
        copy.wait_send()

    @pl.when(top)
    def _():
        for copy in fold:
            copy.wait_send()

    @pl.when(jnp.logical_not(top))
    def _():
        for copy in upward:
            copy.wait_send()

    @pl.when(jnp.logical_not(bottom))
    def _():
        for copy in down:
            copy.wait_send()


def local(tracers, kmt):
    channels = tracers.shape[0]
    chunks = 4
    early = 3
    groups = channels * LEVELS * 2 // LANES
    row_array = VMEM((channels, LEVELS, LANES), jnp.float32)
    packed = VMEM((groups + 1, ROWS, LANES), jnp.float32)
    depth_row = VMEM((1, LANES), jnp.int32)
    anywhere = pl.BlockSpec(memory_space=pl.ANY)
    return pl.pallas_call(
        functools.partial(kernel, channels, chunks, early),
        out_shape=VMEM(tracers.shape, jnp.float32),
        in_specs=[anywhere, anywhere],
        out_specs=pl.BlockSpec(memory_space=VMEM),
        scratch_shapes=[
            VMEM(tracers.shape, jnp.float32),
            VMEM((ROWS, LANES), jnp.int32),
            row_array, row_array, depth_row, depth_row,
            packed, packed, packed,
            VMEM(tracers.shape, jnp.float32),
            VMEM((channels, LEVELS - 1, ROWS, LANES), jnp.float32),
            VMEM((10, LEVELS, ROWS, LANES), jnp.float32),
            VMEM((groups, ROWS, LANES), jnp.float32),
            VMEM((groups, ROWS, LANES), jnp.float32),
            VMEM((4, LEVELS, LANES), jnp.float32),
            pltpu.SemaphoreType.DMA((2,)),
            pltpu.SemaphoreType.DMA((2 * chunks + 6,)),
            pltpu.SemaphoreType.DMA((chunks + 5,)),
        ],
        compiler_params=pltpu.CompilerParams(collective_id=0, has_side_effects=True),
        name="tracer_step",
    )(tracers, kmt)


def solution(mesh):
    return jax.shard_map(
        local,
        mesh=mesh,
        in_specs=(P(None, None, "lat", "lon"), P("lat", "lon")),
        out_specs=P(None, None, "lat", "lon"),
        check_vma=False,
    )
```

```python
import functools

import jax
import jax.numpy as jnp
from jax import lax
from jax.experimental import pallas as pl
from jax.experimental.pallas import tpu as pltpu
from jax.sharding import PartitionSpec as P

THERMAL = 0.2
HALINE = 0.8
REDI_COEF = 0.1
SKEW_COEF = 0.05
SLOPE_MAX = 0.6
SLOPE_WIDTH = 0.2
SLOPE_FLUX = (REDI_COEF - SKEW_COEF) * 0.25
CROSS = (REDI_COEF + SKEW_COEF) * 0.25 / REDI_COEF

ROWS = 8
LANES = 128
LEVELS = 8
SLAB = 16
MESH = pl.DeviceIdType.MESH
VMEM = pltpu.VMEM


def taper(slope):
    return slope * 0.5 * (1.0 + jnp.tanh((SLOPE_MAX - jnp.abs(slope)) / SLOPE_WIDTH))


def slope_of(step, mask, strat_twice):
    return taper(step * mask / jnp.maximum(0.25 * strat_twice, 1.0))


def below(limit, level):
    return jnp.where(level < limit, 1.0, 0.0)


def vertical_pair(values, mask, axis):
    size = values.shape[axis]
    diff = (pltpu.roll(values, size - 1, axis) - values) * mask
    return diff, diff + pltpu.roll(diff, 1, axis)


def tile(tracer, level):
    first = (tracer * LEVELS + level) * ROWS
    return pl.ds(first if isinstance(first, int) else pl.multiple_of(first, ROWS), ROWS)


def rows_of(tracer, row):
    return pl.ds(tracer * LEVELS * ROWS + row, LEVELS, stride=ROWS)


def up_one(values, axis):
    return pltpu.roll(values, values.shape[axis] - 1, axis)


def kernel(
    channels, chunks, early, tracers, flat, kmt, out,
    field, row_south, row_north, depth, from_south, from_north, depth_south, depth_north,
    sides, from_west, from_east,
    main, cross_x, coef, inner, edge, row_coef,
    load_sem, send_sem, recv_sem,
):
    lon, lat = lax.axis_index("lon"), lax.axis_index("lat")
    blocks, bands = lax.axis_size("lon"), lax.axis_size("lat")
    top, bottom = lat == bands - 1, lat == 0
    west = (lax.rem(lon + blocks - 1, blocks), lat)
    east = (lax.rem(lon + 1, blocks), lat)
    north = (jnp.where(top, blocks - 1 - lon, lon), jnp.where(top, lat, lat + 1))
    south = (lon, jnp.maximum(lat - 1, 0))
    patient = jnp.logical_or(lax.rem(lon, SLAB) == 0, jnp.logical_and(top, lax.rem(lon, SLAB) < SLAB // 2 - 1))
    per_chunk = channels // chunks
    per_group = LANES // 2 // LEVELS
    groups = channels // per_group

    barrier = pltpu.get_barrier_semaphore()
    for other in (north, west, east):
        pl.semaphore_signal(barrier, inc=1, device_id=other, device_id_type=MESH)

    @pl.when(jnp.logical_not(bottom))
    def _():
        pl.semaphore_signal(barrier, inc=1, device_id=south, device_id_type=MESH)

    rows_load = [
        pltpu.make_async_copy(tracers.at[:, :, ROWS - 1, :], row_north, load_sem.at[groups]),
        pltpu.make_async_copy(tracers.at[:, :, 0, :], row_south, load_sem.at[groups + 1]),
    ]
    depth_load = pltpu.make_async_copy(kmt, depth, load_sem.at[groups + 2])
    part = per_group * LEVELS * ROWS
    loads = [
        pltpu.make_async_copy(
            flat.at[pl.ds(group * part, part)], field.at[pl.ds(group * part, part)], load_sem.at[group]
        )
        for group in range(groups)
    ]
    depth_load.start()
    rows_load[0].start()
    for load in loads:
        load.start()
    rows_load[1].start()

    def send(source, target, slot, device, send_slot=None):
        return pltpu.make_async_remote_copy(
            src_ref=source,
            dst_ref=target,
            send_sem=send_sem.at[slot if send_slot is None else send_slot],
            recv_sem=recv_sem.at[slot],
            device_id=device,
            device_id_type=MESH,
        )

    def to_north_halo(own_row, values, device, first_send):
        copies = [send(depth.at[pl.ds(own_row, 1)], depth_north, 0, device, first_send)]
        for chunk in range(chunks):
            span = pl.ds(chunk * per_chunk, per_chunk)
            slot = 1 + chunk
            copies.append(send(values.at[span], from_north.at[span], slot, device, first_send + slot))
        return copies

    base = 1 + chunks
    fold = to_north_halo(ROWS - 1, row_north, north, base + 4)
    down = to_north_halo(0, row_south, south, 0)
    upward = [
        send(depth.at[pl.ds(ROWS - 1, 1)], depth_south, base, north),
        send(row_north, from_south, base + 1, north),
    ]
    across = [
        send(sides, from_east, base + 2, west),
        send(sides, from_west, base + 3, east),
    ]

    shape = (ROWS, LANES)
    lane = lax.broadcasted_iota(jnp.int32, shape, 1)
    row = lax.broadcasted_iota(jnp.int32, shape, 0)
    zero = jnp.zeros(shape, jnp.float32)

    def right(values, count=1):
        return pltpu.roll(values, count % LANES, 1)

    def wide(values):
        return jnp.broadcast_to(values, shape)

    pair_id = lax.rem(lane + 1, LANES) // 2
    at_edge = jnp.logical_or(lane == 0, lane == LANES - 1)

    def pack_columns():
        sides[groups] = depth[...].astype(jnp.float32)
        for group in range(groups):
            loads[group].wait()
            packed = zero
            for at in range(LANES // 2):
                tracer, k = group * per_group + at // LEVELS, at % LEVELS
                packed = jnp.where(pair_id == at, right(field[tile(tracer, k)], 2 * at), packed)
            sides[group] = packed

    def own_faces():
        depth_here = depth[...]
        density = [HALINE * field[tile(1, k)] - THERMAL * field[tile(0, k)] for k in range(LEVELS)]
        level_mask = [below(depth_here, k + 1) for k in range(LEVELS - 1)]
        strat_face = [(density[k + 1] - density[k]) * level_mask[k] for k in range(LEVELS - 1)]
        strat = [strat_face[0]]
        strat += [strat_face[k - 1] + strat_face[k] for k in range(1, LEVELS - 1)]
        strat += [strat_face[LEVELS - 2]]
        depth_left = jnp.minimum(depth_here, jnp.where(lane == 0, 0, right(depth_here)))
        depth_right = jnp.minimum(depth_here, jnp.where(lane == LANES - 1, 0, right(depth_here, -1)))
        depth_down = jnp.minimum(depth_here, jnp.where(row == 0, 0, pltpu.roll(depth_here, 1, 0)))
        inner_lanes = jnp.where(at_edge, 0.0, 1.0)
        inner_rows = jnp.where(jnp.logical_or(row == 0, row == ROWS - 1), 0.0, 1.0)
        sum_x, sum_y = [], []
        inner_slope = zero
        for k in range(LEVELS):
            mask_w, mask_e, mask_s = (below(limit, k) for limit in (depth_left, depth_right, depth_down))
            slope_w = slope_of(density[k] - right(density[k]), mask_w, strat[k] + right(strat[k]))
            slope_e = slope_of(right(density[k], -1) - density[k], mask_e, strat[k] + right(strat[k], -1))
            slope_s = slope_of(
                density[k] - pltpu.roll(density[k], 1, 0), mask_s, strat[k] + pltpu.roll(strat[k], 1, 0)
            )
            coef[0, k] = REDI_COEF * mask_w
            coef[1, k] = REDI_COEF * mask_e
            coef[2, k] = REDI_COEF * mask_s
            coef[3, k] = SLOPE_FLUX * slope_w
            coef[4, k] = SLOPE_FLUX * slope_e
            coef[5, k] = SLOPE_FLUX * slope_s
            coef[6, k] = level_mask[k] if k < LEVELS - 1 else zero
            sum_x.append(slope_w + slope_e)
            sum_y.append(slope_s + up_one(slope_s, 0))
            inner_slope = jnp.where(pair_id == k, right(sum_x[k], 2 * k), inner_slope)
            row_coef[0, pl.ds(k, 1)] = slope_s[1:2]
            row_coef[1, pl.ds(k, 1)] = REDI_COEF * mask_s[1:2]
            row_coef[2, pl.ds(k, 1)] = slope_s[ROWS - 1 : ROWS]
            row_coef[3, pl.ds(k, 1)] = REDI_COEF * mask_s[ROWS - 1 : ROWS]
        for k in range(LEVELS - 1):
            mean_x = 0.25 * (sum_x[k] + sum_x[k + 1]) * inner_lanes
            mean_y = 0.25 * (sum_y[k] + sum_y[k + 1]) * inner_rows
            coef[7, k] = CROSS * mean_x * level_mask[k]
            coef[8, k] = CROSS * mean_y * level_mask[k]
            coef[9, k] = REDI_COEF * (mean_x * mean_x + mean_y * mean_y)

        def one_group(group, carry):
            for slot in range(per_group):
                tracer = group * per_group + slot
                values = [field[tile(tracer, k)] for k in range(LEVELS)]
                diff = [(values[k + 1] - values[k]) * coef[6, k] for k in range(LEVELS - 1)]
                pair = [diff[0]] + [diff[k - 1] + diff[k] for k in range(1, LEVELS - 1)] + [diff[LEVELS - 2]]
                grad_x, grad_y, total = [], [], []
                for k in range(LEVELS):
                    here, both = values[k], pair[k]
                    grad_w = coef[0, k] * (here - right(here))
                    grad_e = coef[1, k] * (right(here, -1) - here)
                    grad_s = coef[2, k] * (here - pltpu.roll(here, 1, 0))
                    flux_w = grad_w + coef[3, k] * (both + right(both))
                    flux_e = grad_e + coef[4, k] * (both + right(both, -1))
                    flux_s = grad_s + coef[5, k] * (both + pltpu.roll(both, 1, 0))
                    grad_x.append(grad_w + grad_e)
                    grad_y.append(grad_s + up_one(grad_s, 0))
                    total.append(here + (flux_e - flux_w) + (up_one(flux_s, 0) - flux_s))
                above = None
                for k in range(LEVELS):
                    added = total[k] if above is None else total[k] - above
                    if k < LEVELS - 1:
                        both_x, both_y = grad_x[k] + grad_x[k + 1], grad_y[k] + grad_y[k + 1]
                        cross_x[tracer, k] = both_x
                        above = coef[7, k] * both_x + coef[8, k] * both_y + coef[9, k] * diff[k]
                        added = added + above
                    main[tile(tracer, k)] = added
            return carry

        coef[7, LEVELS - 1] = inner_slope
        lax.fori_loop(0, groups, one_group, 0)

        for group in range(groups):
            packed = zero
            for at in range(LANES // 2):
                tracer, k = group * per_group + at // LEVELS, at % LEVELS
                if k < LEVELS - 1:
                    packed = jnp.where(pair_id == at, right(cross_x[tracer, k], 2 * at), packed)
            inner[group] = packed

    def start_rows():
        for load in rows_load[1:]:
            load.wait()

        @pl.when(jnp.logical_not(bottom))
        def _():
            for copy in down:
                copy.start()

        @pl.when(jnp.logical_not(top))
        def _():
            for copy in upward:
                copy.start()

    def start_columns():
        for copy in across:
            copy.start()

    def start_fold(copies):
        for copy in copies:
            copy.start()

    slab_at = lax.rem(lon, SLAB)
    yielding = jnp.logical_and(top, jnp.logical_or(slab_at == SLAB - 4, slab_at == SLAB - 3))
    eager = jnp.logical_and(top, jnp.logical_not(jnp.logical_or(patient, yielding)))
    depth_load.wait()
    rows_load[0].wait()

    @pl.when(patient)
    def _():
        pack_columns()
        own_faces()

    pl.semaphore_wait(barrier, jnp.where(bottom, 3, 4))

    @pl.when(patient)
    def _():
        start_rows()
        start_columns()
        pl.when(top)(functools.partial(start_fold, fold))

    @pl.when(jnp.logical_not(patient))
    def _():
        pl.when(eager)(functools.partial(start_fold, fold[:early]))
        pack_columns()
        start_columns()
        start_rows()
        pl.when(eager)(functools.partial(start_fold, fold[early:]))
        own_faces()
        pl.when(yielding)(functools.partial(start_fold, fold))

    @pl.when(bottom)
    def _():
        from_south[...] = jnp.zeros_like(from_south)
        depth_south[...] = jnp.zeros_like(depth_south)

    depth_here = depth[...]
    inner_slope = coef[7, LEVELS - 1]

    source_lane = jnp.where(top, LANES - 1 - lane, lane)

    def mirrored(values):
        return jnp.take_along_axis(values, source_lane, axis=1, mode="promise_in_bounds")

    def row_terms(at, own_row, beyond, depth_beyond, arranged, first):
        sign = 1.0 if at else -1.0
        beside_row = at - 1 if at else 1
        limit = wide(depth_here[at : at + 1])
        mask = below(limit, row + 1)
        limit_beyond = arranged(wide(depth_beyond[...]))
        mask_beyond = below(limit_beyond, row + 1)
        face = below(jnp.minimum(limit, limit_beyond), row)
        density_row = HALINE * own_row[1] - THERMAL * own_row[0]
        density_beyond = arranged(HALINE * beyond[1] - THERMAL * beyond[0])
        slope = slope_of(
            sign * (density_beyond - density_row),
            face,
            vertical_pair(density_row, mask, 0)[1] + vertical_pair(density_beyond, mask_beyond, 0)[1],
        )
        sums = slope + row_coef[first]
        mean = 0.25 * (sums + up_one(sums, 0))
        cross, square = CROSS * mean * mask, REDI_COEF * mean * mean
        grad_face, flux_face, grad_in = REDI_COEF * face, sign * SLOPE_FLUX * slope, row_coef[first + 1]

        def add(tracer):
            own, other = own_row[tracer], arranged(beyond[tracer])
            step = grad_face * (other - own)
            diff, pair = vertical_pair(own, mask, 0)
            both = pair + vertical_pair(other, mask_beyond, 0)[1]
            grads = sign * (step + grad_in * (own - field[rows_of(tracer, beside_row)]))
            vertical = cross * (grads + up_one(grads, 0)) + square * diff
            change = vertical - pltpu.roll(vertical, 1, 0) + (step + flux_face * both)
            out[rows_of(tracer, at)] = out[rows_of(tracer, at)] + change

        return add

    even = lax.rem(lane, 2) == 0
    side_level = lax.rem(pair_id, LEVELS)
    side_sign = jnp.where(even, -1.0, 1.0)
    span = 2 * LEVELS

    def beside(group, shift=0):
        return jnp.where(even, right(from_west[group], 1 - shift), right(from_east[group], -1 - shift))

    def side_pair(values, mask):
        diff = (right(values, -2) - values) * mask
        return diff, diff + right(diff, 2)

    def every_tracer(values):
        values = jnp.where(pair_id < LEVELS, values, 0.0)
        total = values
        for shift in range(span, LANES, span):
            total = total + right(values, shift)
        return total

    here_limit = jnp.where(even, wide(depth_here[:, 0:1]), wide(depth_here[:, LANES - 1 : LANES]))
    here_mask = below(here_limit, side_level + 1)
    density_side = HALINE * right(sides[0], -span) - THERMAL * sides[0]
    strat_side = side_pair(density_side, here_mask)[1]

    for copy in across:
        copy.wait_recv()

    west_limit = wide(from_west[groups][:, LANES - 1 : LANES]).astype(jnp.int32)
    east_limit = wide(from_east[groups][:, 0:1]).astype(jnp.int32)
    there_limit = jnp.where(even, west_limit, east_limit)
    there_mask = below(there_limit, side_level + 1)
    side_mask = below(jnp.minimum(there_limit, here_limit), side_level)
    density_there = HALINE * beside(0, span) - THERMAL * beside(0)
    side_slope = slope_of(
        side_sign * (density_there - density_side),
        side_mask,
        strat_side + side_pair(density_there, there_mask)[1],
    )
    sums = side_slope + inner_slope
    mean = 0.25 * (sums + right(sums, -2))
    side_flux = every_tracer(SLOPE_FLUX * side_sign * side_slope)
    side_mean = every_tracer(mean)
    side_cross = CROSS * side_mean * here_mask
    side_square = REDI_COEF * side_mean * side_mean
    side_grad = REDI_COEF * side_mask
    for group in range(groups):
        own, other = sides[group], beside(group)
        step = side_grad * (other - own)
        diff, pair = side_pair(own, here_mask)
        grads = inner[group] + side_sign * (step + right(step, -2))
        vertical = side_cross * grads + side_square * diff
        change = vertical - right(vertical, 2) + step + side_flux * (pair + side_pair(other, there_mask)[1])
        edge[group] = change
    for group in range(groups):
        change = edge[group]
        for at in range(LANES // 2):
            tracer, k = group * per_group + at // LEVELS, at % LEVELS
            out[tile(tracer, k)] = main[tile(tracer, k)] + jnp.where(at_edge, right(change, -2 * at), 0.0)

    @pl.when(jnp.logical_not(bottom))
    def _():
        for copy in upward:
            copy.wait_recv()

    add_south = row_terms(0, row_south, from_south, depth_south, lambda values: values, 0)
    for tracer in range(channels):
        add_south(tracer)

    for copy in down[:2]:
        copy.wait_recv()
    add_north = row_terms(ROWS - 1, row_north, from_north, depth_north, mirrored, 2)
    for chunk in range(chunks):
        if chunk:
            down[1 + chunk].wait_recv()
        for tracer in range(chunk * per_chunk, (chunk + 1) * per_chunk):
            add_north(tracer)


    for copy in across:
        copy.wait_send()

    @pl.when(top)
    def _():
        for copy in fold:
            copy.wait_send()

    @pl.when(jnp.logical_not(top))
    def _():
        for copy in upward:
            copy.wait_send()

    @pl.when(jnp.logical_not(bottom))
    def _():
        for copy in down:
            copy.wait_send()


def local(tracers, kmt):
    channels = tracers.shape[0]
    chunks = 4
    early = 2
    groups = channels * LEVELS * 2 // LANES
    row_array = VMEM((channels, LEVELS, LANES), jnp.float32)
    packed = VMEM((groups + 1, ROWS, LANES), jnp.float32)
    depth_row = VMEM((1, LANES), jnp.int32)
    anywhere = pl.BlockSpec(memory_space=pl.ANY)
    flat = tracers.reshape(-1, LANES)
    updated = pl.pallas_call(
        functools.partial(kernel, channels, chunks, early),
        out_shape=VMEM(flat.shape, jnp.float32),
        in_specs=[anywhere, anywhere, anywhere],
        out_specs=pl.BlockSpec(memory_space=VMEM),
        scratch_shapes=[
            VMEM(flat.shape, jnp.float32),
            row_array, row_array, VMEM((ROWS, LANES), jnp.int32),
            row_array, row_array, depth_row, depth_row,
            packed, packed, packed,
            VMEM(flat.shape, jnp.float32),
            VMEM((channels, LEVELS - 1, ROWS, LANES), jnp.float32),
            VMEM((10, LEVELS, ROWS, LANES), jnp.float32),
            VMEM((groups, ROWS, LANES), jnp.float32),
            VMEM((groups, ROWS, LANES), jnp.float32),
            VMEM((4, LEVELS, LANES), jnp.float32),
            pltpu.SemaphoreType.DMA((groups + 3,)),
            pltpu.SemaphoreType.DMA((2 * chunks + 6,)),
            pltpu.SemaphoreType.DMA((chunks + 5,)),
        ],
        compiler_params=pltpu.CompilerParams(collective_id=0, has_side_effects=True),
        name="tracer_step",
    )(tracers, flat, kmt)
    return updated.reshape(tracers.shape)


def solution(mesh):
    return jax.shard_map(
        local,
        mesh=mesh,
        in_specs=(P(None, None, "lat", "lon"), P("lat", "lon")),
        out_specs=P(None, None, "lat", "lon"),
        check_vma=False,
    )
```

```python
import functools

import jax
import jax.numpy as jnp
from jax import lax
from jax.experimental import pallas as pl
from jax.experimental.pallas import tpu as pltpu
from jax.sharding import PartitionSpec as P

THERMAL = 0.2
HALINE = 0.8
REDI_COEF = 0.1
SKEW_COEF = 0.05
SLOPE_MAX = 0.6
SLOPE_WIDTH = 0.2
SLOPE_FLUX = (REDI_COEF - SKEW_COEF) * 0.25
CROSS = (REDI_COEF + SKEW_COEF) * 0.25 / REDI_COEF

ROWS = 8
LANES = 128
LEVELS = 8
SLAB = 16
MESH = pl.DeviceIdType.MESH
VMEM = pltpu.VMEM


def taper(slope):
    return slope * 0.5 * (1.0 + jnp.tanh((SLOPE_MAX - jnp.abs(slope)) / SLOPE_WIDTH))


def slope_of(step, mask, strat_twice):
    return taper(step * mask / jnp.maximum(0.25 * strat_twice, 1.0))


def below(limit, level):
    return jnp.where(level < limit, 1.0, 0.0)


def vertical_pair(values, mask, axis):
    size = values.shape[axis]
    diff = (pltpu.roll(values, size - 1, axis) - values) * mask
    return diff, diff + pltpu.roll(diff, 1, axis)


def tile(tracer, level):
    first = (tracer * LEVELS + level) * ROWS
    return pl.ds(first if isinstance(first, int) else pl.multiple_of(first, ROWS), ROWS)


def rows_of(tracer, row):
    return pl.ds(tracer * LEVELS * ROWS + row, LEVELS, stride=ROWS)


def up_one(values, axis):
    return pltpu.roll(values, values.shape[axis] - 1, axis)


def kernel(
    channels, chunks, early, tracers, flat, kmt, out,
    field, row_south, row_north, depth, from_south, from_north, depth_south, depth_north,
    sides, from_west, from_east,
    main, cross_x, coef, inner, edge, row_coef,
    load_sem, send_sem, recv_sem, ready,
):
    lon, lat = lax.axis_index("lon"), lax.axis_index("lat")
    blocks, bands = lax.axis_size("lon"), lax.axis_size("lat")
    top, bottom = lat == bands - 1, lat == 0
    west = (lax.rem(lon + blocks - 1, blocks), lat)
    east = (lax.rem(lon + 1, blocks), lat)
    north = (jnp.where(top, blocks - 1 - lon, lon), jnp.where(top, lat, lat + 1))
    south = (lon, jnp.maximum(lat - 1, 0))
    patient = jnp.logical_or(lax.rem(lon, SLAB) == 0, jnp.logical_and(top, lax.rem(lon, SLAB) < SLAB // 2 - 1))
    per_chunk = channels // chunks
    per_group = LANES // 2 // LEVELS
    groups = channels // per_group

    slab_at = lax.rem(lon, SLAB)
    opening = jnp.logical_and(slab_at == 0, jnp.logical_not(top))
    closing = jnp.logical_and(slab_at == SLAB - 1, jnp.logical_not(top))

    barrier = pltpu.get_barrier_semaphore()
    for other in (north, west):
        pl.semaphore_signal(barrier, inc=1, device_id=other, device_id_type=MESH)

    @pl.when(jnp.logical_not(closing))
    def _():
        pl.semaphore_signal(barrier, inc=1, device_id=east, device_id_type=MESH)

    @pl.when(jnp.logical_not(bottom))
    def _():
        pl.semaphore_signal(barrier, inc=1, device_id=south, device_id_type=MESH)

    rows_load = [
        pltpu.make_async_copy(tracers.at[:, :, ROWS - 1, :], row_north, load_sem.at[groups]),
        pltpu.make_async_copy(tracers.at[:, :, 0, :], row_south, load_sem.at[groups + 1]),
    ]
    depth_load = pltpu.make_async_copy(kmt, depth, load_sem.at[groups + 2])
    part = per_group * LEVELS * ROWS
    loads = [
        pltpu.make_async_copy(
            flat.at[pl.ds(group * part, part)], field.at[pl.ds(group * part, part)], load_sem.at[group]
        )
        for group in range(groups)
    ]
    depth_load.start()
    rows_load[0].start()
    for load in loads:
        load.start()
    rows_load[1].start()

    def send(source, target, slot, device, send_slot=None):
        return pltpu.make_async_remote_copy(
            src_ref=source,
            dst_ref=target,
            send_sem=send_sem.at[slot if send_slot is None else send_slot],
            recv_sem=recv_sem.at[slot],
            device_id=device,
            device_id_type=MESH,
        )

    def to_north_halo(own_row, values, device, first_send):
        copies = [send(depth.at[pl.ds(own_row, 1)], depth_north, 0, device, first_send)]
        for chunk in range(chunks):
            span = pl.ds(chunk * per_chunk, per_chunk)
            slot = 1 + chunk
            copies.append(send(values.at[span], from_north.at[span], slot, device, first_send + slot))
        return copies

    base = 1 + chunks
    fold = to_north_halo(ROWS - 1, row_north, north, base + 4)
    down = to_north_halo(0, row_south, south, 0)
    upward = [
        send(depth.at[pl.ds(ROWS - 1, 1)], depth_south, base, north),
        send(row_north, from_south, base + 1, north),
    ]
    across = [
        send(sides, from_east, base + 2, west),
        send(sides, from_west, base + 3, east),
    ]

    shape = (ROWS, LANES)
    lane = lax.broadcasted_iota(jnp.int32, shape, 1)
    row = lax.broadcasted_iota(jnp.int32, shape, 0)
    zero = jnp.zeros(shape, jnp.float32)

    def right(values, count=1):
        return pltpu.roll(values, count % LANES, 1)

    def wide(values):
        return jnp.broadcast_to(values, shape)

    pair_id = lax.rem(lane + 1, LANES) // 2
    at_edge = jnp.logical_or(lane == 0, lane == LANES - 1)

    def pack_columns():
        sides[groups] = depth[...].astype(jnp.float32)
        for group in range(groups):
            loads[group].wait()
            packed = zero
            for at in range(LANES // 2):
                tracer, k = group * per_group + at // LEVELS, at % LEVELS
                packed = jnp.where(pair_id == at, right(field[tile(tracer, k)], 2 * at), packed)
            sides[group] = packed

    def own_faces():
        depth_here = depth[...]
        density = [HALINE * field[tile(1, k)] - THERMAL * field[tile(0, k)] for k in range(LEVELS)]
        level_mask = [below(depth_here, k + 1) for k in range(LEVELS - 1)]
        strat_face = [(density[k + 1] - density[k]) * level_mask[k] for k in range(LEVELS - 1)]
        strat = [strat_face[0]]
        strat += [strat_face[k - 1] + strat_face[k] for k in range(1, LEVELS - 1)]
        strat += [strat_face[LEVELS - 2]]
        depth_left = jnp.minimum(depth_here, jnp.where(lane == 0, 0, right(depth_here)))
        depth_right = jnp.minimum(depth_here, jnp.where(lane == LANES - 1, 0, right(depth_here, -1)))
        depth_down = jnp.minimum(depth_here, jnp.where(row == 0, 0, pltpu.roll(depth_here, 1, 0)))
        inner_lanes = jnp.where(at_edge, 0.0, 1.0)
        inner_rows = jnp.where(jnp.logical_or(row == 0, row == ROWS - 1), 0.0, 1.0)
        sum_x, sum_y = [], []
        inner_slope = zero
        for k in range(LEVELS):
            mask_w, mask_e, mask_s = (below(limit, k) for limit in (depth_left, depth_right, depth_down))
            slope_w = slope_of(density[k] - right(density[k]), mask_w, strat[k] + right(strat[k]))
            slope_e = slope_of(right(density[k], -1) - density[k], mask_e, strat[k] + right(strat[k], -1))
            slope_s = slope_of(
                density[k] - pltpu.roll(density[k], 1, 0), mask_s, strat[k] + pltpu.roll(strat[k], 1, 0)
            )
            coef[0, k] = REDI_COEF * mask_w
            coef[1, k] = REDI_COEF * mask_e
            coef[2, k] = REDI_COEF * mask_s
            coef[3, k] = SLOPE_FLUX * slope_w
            coef[4, k] = SLOPE_FLUX * slope_e
            coef[5, k] = SLOPE_FLUX * slope_s
            coef[6, k] = level_mask[k] if k < LEVELS - 1 else zero
            sum_x.append(slope_w + slope_e)
            sum_y.append(slope_s + up_one(slope_s, 0))
            inner_slope = jnp.where(pair_id == k, right(sum_x[k], 2 * k), inner_slope)
            row_coef[0, pl.ds(k, 1)] = slope_s[1:2]
            row_coef[1, pl.ds(k, 1)] = REDI_COEF * mask_s[1:2]
            row_coef[2, pl.ds(k, 1)] = slope_s[ROWS - 1 : ROWS]
            row_coef[3, pl.ds(k, 1)] = REDI_COEF * mask_s[ROWS - 1 : ROWS]
        for k in range(LEVELS - 1):
            mean_x = 0.25 * (sum_x[k] + sum_x[k + 1]) * inner_lanes
            mean_y = 0.25 * (sum_y[k] + sum_y[k + 1]) * inner_rows
            coef[7, k] = CROSS * mean_x * level_mask[k]
            coef[8, k] = CROSS * mean_y * level_mask[k]
            coef[9, k] = REDI_COEF * (mean_x * mean_x + mean_y * mean_y)

        def one_group(group, carry):
            for slot in range(per_group):
                tracer = group * per_group + slot
                values = [field[tile(tracer, k)] for k in range(LEVELS)]
                diff = [(values[k + 1] - values[k]) * coef[6, k] for k in range(LEVELS - 1)]
                pair = [diff[0]] + [diff[k - 1] + diff[k] for k in range(1, LEVELS - 1)] + [diff[LEVELS - 2]]
                grad_x, grad_y, total = [], [], []
                for k in range(LEVELS):
                    here, both = values[k], pair[k]
                    grad_w = coef[0, k] * (here - right(here))
                    grad_e = coef[1, k] * (right(here, -1) - here)
                    grad_s = coef[2, k] * (here - pltpu.roll(here, 1, 0))
                    flux_w = grad_w + coef[3, k] * (both + right(both))
                    flux_e = grad_e + coef[4, k] * (both + right(both, -1))
                    flux_s = grad_s + coef[5, k] * (both + pltpu.roll(both, 1, 0))
                    grad_x.append(grad_w + grad_e)
                    grad_y.append(grad_s + up_one(grad_s, 0))
                    total.append(here + (flux_e - flux_w) + (up_one(flux_s, 0) - flux_s))
                above = None
                for k in range(LEVELS):
                    added = total[k] if above is None else total[k] - above
                    if k < LEVELS - 1:
                        both_x, both_y = grad_x[k] + grad_x[k + 1], grad_y[k] + grad_y[k + 1]
                        cross_x[tracer, k] = both_x
                        above = coef[7, k] * both_x + coef[8, k] * both_y + coef[9, k] * diff[k]
                        added = added + above
                    main[tile(tracer, k)] = added
            return carry

        coef[7, LEVELS - 1] = inner_slope
        lax.fori_loop(0, groups, one_group, 0)

        for group in range(groups):
            packed = zero
            for at in range(LANES // 2):
                tracer, k = group * per_group + at // LEVELS, at % LEVELS
                if k < LEVELS - 1:
                    packed = jnp.where(pair_id == at, right(cross_x[tracer, k], 2 * at), packed)
            inner[group] = packed

    def start_rows():
        for load in rows_load[1:]:
            load.wait()

        @pl.when(jnp.logical_not(bottom))
        def _():
            for copy in down:
                copy.start()

        @pl.when(jnp.logical_not(top))
        def _():
            for copy in upward:
                copy.start()

    def start_columns():
        across[1].start()
        pl.when(jnp.logical_not(opening))(across[0].start)

    def start_fold(copies):
        for copy in copies:
            copy.start()

    yielding = jnp.logical_and(top, jnp.logical_or(slab_at == SLAB - 4, slab_at == SLAB - 3))
    eager = jnp.logical_and(top, jnp.logical_not(jnp.logical_or(patient, yielding)))
    depth_load.wait()
    rows_load[0].wait()

    @pl.when(patient)
    def _():
        pack_columns()
        own_faces()

    pl.semaphore_wait(barrier, jnp.where(bottom, 3, 4) - jnp.where(opening, 1, 0))

    @pl.when(closing)
    def _():
        pl.semaphore_signal(ready, inc=1, device_id=east, device_id_type=MESH)

    @pl.when(patient)
    def _():
        start_rows()
        start_columns()
        pl.when(top)(functools.partial(start_fold, fold))

    @pl.when(jnp.logical_not(patient))
    def _():
        pl.when(eager)(functools.partial(start_fold, fold[:early]))
        pack_columns()
        start_columns()
        pl.when(eager)(functools.partial(start_fold, fold[early:]))
        start_rows()
        nearer = jnp.logical_and(yielding, slab_at == SLAB - 3)
        pl.when(nearer)(functools.partial(start_fold, fold[:early]))
        own_faces()
        pl.when(jnp.logical_and(yielding, slab_at == SLAB - 4))(functools.partial(start_fold, fold[:early]))
        pl.when(yielding)(functools.partial(start_fold, fold[early:]))

    @pl.when(bottom)
    def _():
        from_south[...] = jnp.zeros_like(from_south)
        depth_south[...] = jnp.zeros_like(depth_south)

    depth_here = depth[...]
    inner_slope = coef[7, LEVELS - 1]

    source_lane = jnp.where(top, LANES - 1 - lane, lane)

    def mirrored(values):
        return jnp.take_along_axis(values, source_lane, axis=1, mode="promise_in_bounds")

    def row_terms(at, own_row, beyond, depth_beyond, arranged, first):
        sign = 1.0 if at else -1.0
        beside_row = at - 1 if at else 1
        limit = wide(depth_here[at : at + 1])
        mask = below(limit, row + 1)
        limit_beyond = arranged(wide(depth_beyond[...]))
        mask_beyond = below(limit_beyond, row + 1)
        face = below(jnp.minimum(limit, limit_beyond), row)
        density_row = HALINE * own_row[1] - THERMAL * own_row[0]
        density_beyond = arranged(HALINE * beyond[1] - THERMAL * beyond[0])
        slope = slope_of(
            sign * (density_beyond - density_row),
            face,
            vertical_pair(density_row, mask, 0)[1] + vertical_pair(density_beyond, mask_beyond, 0)[1],
        )
        sums = slope + row_coef[first]
        mean = 0.25 * (sums + up_one(sums, 0))
        cross, square = CROSS * mean * mask, REDI_COEF * mean * mean
        grad_face, flux_face, grad_in = REDI_COEF * face, sign * SLOPE_FLUX * slope, row_coef[first + 1]

        def add(tracer, result):
            own, other = own_row[tracer], arranged(beyond[tracer])
            step = grad_face * (other - own)
            diff, pair = vertical_pair(own, mask, 0)
            both = pair + vertical_pair(other, mask_beyond, 0)[1]
            grads = sign * (step + grad_in * (own - field[rows_of(tracer, beside_row)]))
            vertical = cross * (grads + up_one(grads, 0)) + square * diff
            change = vertical - pltpu.roll(vertical, 1, 0) + (step + flux_face * both)
            result[rows_of(tracer, at)] = result[rows_of(tracer, at)] + change

        return add

    @pl.when(jnp.logical_not(bottom))
    def _():
        for copy in upward:
            copy.wait_recv()

    add_south = row_terms(0, row_south, from_south, depth_south, lambda values: values, 0)
    for tracer in range(channels):
        add_south(tracer, main)

    def north_face(result):
        for copy in down[:2]:
            copy.wait_recv()
        add_north = row_terms(ROWS - 1, row_north, from_north, depth_north, mirrored, 2)
        for chunk in range(chunks):
            if chunk:
                down[1 + chunk].wait_recv()
            for tracer in range(chunk * per_chunk, (chunk + 1) * per_chunk):
                add_north(tracer, result)

    pl.when(jnp.logical_not(top))(functools.partial(north_face, main))

    @pl.when(opening)
    def _():
        pl.semaphore_wait(ready, 1)
        across[0].start()

    even = lax.rem(lane, 2) == 0
    side_level = lax.rem(pair_id, LEVELS)
    side_sign = jnp.where(even, -1.0, 1.0)
    span = 2 * LEVELS

    def beside(group, shift=0):
        return jnp.where(even, right(from_west[group], 1 - shift), right(from_east[group], -1 - shift))

    def side_pair(values, mask):
        diff = (right(values, -2) - values) * mask
        return diff, diff + right(diff, 2)

    def every_tracer(values):
        values = jnp.where(pair_id < LEVELS, values, 0.0)
        total = values
        for shift in range(span, LANES, span):
            total = total + right(values, shift)
        return total

    here_limit = jnp.where(even, wide(depth_here[:, 0:1]), wide(depth_here[:, LANES - 1 : LANES]))
    here_mask = below(here_limit, side_level + 1)
    density_side = HALINE * right(sides[0], -span) - THERMAL * sides[0]
    strat_side = side_pair(density_side, here_mask)[1]

    for copy in across:
        copy.wait_recv()

    west_limit = wide(from_west[groups][:, LANES - 1 : LANES]).astype(jnp.int32)
    east_limit = wide(from_east[groups][:, 0:1]).astype(jnp.int32)
    there_limit = jnp.where(even, west_limit, east_limit)
    there_mask = below(there_limit, side_level + 1)
    side_mask = below(jnp.minimum(there_limit, here_limit), side_level)
    density_there = HALINE * beside(0, span) - THERMAL * beside(0)
    side_slope = slope_of(
        side_sign * (density_there - density_side),
        side_mask,
        strat_side + side_pair(density_there, there_mask)[1],
    )
    sums = side_slope + inner_slope
    mean = 0.25 * (sums + right(sums, -2))
    side_flux = every_tracer(SLOPE_FLUX * side_sign * side_slope)
    side_mean = every_tracer(mean)
    side_cross = CROSS * side_mean * here_mask
    side_square = REDI_COEF * side_mean * side_mean
    side_grad = REDI_COEF * side_mask
    for group in range(groups):
        own, other = sides[group], beside(group)
        step = side_grad * (other - own)
        diff, pair = side_pair(own, here_mask)
        grads = inner[group] + side_sign * (step + right(step, -2))
        vertical = side_cross * grads + side_square * diff
        change = vertical - right(vertical, 2) + step + side_flux * (pair + side_pair(other, there_mask)[1])
        edge[group] = change
    for group in range(groups):
        change = edge[group]
        for at in range(LANES // 2):
            tracer, k = group * per_group + at // LEVELS, at % LEVELS
            out[tile(tracer, k)] = main[tile(tracer, k)] + jnp.where(at_edge, right(change, -2 * at), 0.0)

    pl.when(top)(functools.partial(north_face, out))

    for copy in across:
        copy.wait_send()

    @pl.when(top)
    def _():
        for copy in fold:
            copy.wait_send()

    @pl.when(jnp.logical_not(top))
    def _():
        for copy in upward:
            copy.wait_send()

    @pl.when(jnp.logical_not(bottom))
    def _():
        for copy in down:
            copy.wait_send()


def local(tracers, kmt):
    channels = tracers.shape[0]
    chunks = 4
    early = 2
    groups = channels * LEVELS * 2 // LANES
    row_array = VMEM((channels, LEVELS, LANES), jnp.float32)
    packed = VMEM((groups + 1, ROWS, LANES), jnp.float32)
    depth_row = VMEM((1, LANES), jnp.int32)
    anywhere = pl.BlockSpec(memory_space=pl.ANY)
    flat = tracers.reshape(-1, LANES)
    updated = pl.pallas_call(
        functools.partial(kernel, channels, chunks, early),
        out_shape=VMEM(flat.shape, jnp.float32),
        in_specs=[anywhere, anywhere, anywhere],
        out_specs=pl.BlockSpec(memory_space=VMEM),
        scratch_shapes=[
            VMEM(flat.shape, jnp.float32),
            row_array, row_array, VMEM((ROWS, LANES), jnp.int32),
            row_array, row_array, depth_row, depth_row,
            packed, packed, packed,
            VMEM(flat.shape, jnp.float32),
            VMEM((channels, LEVELS - 1, ROWS, LANES), jnp.float32),
            VMEM((10, LEVELS, ROWS, LANES), jnp.float32),
            VMEM((groups, ROWS, LANES), jnp.float32),
            VMEM((groups, ROWS, LANES), jnp.float32),
            VMEM((4, LEVELS, LANES), jnp.float32),
            pltpu.SemaphoreType.DMA((groups + 3,)),
            pltpu.SemaphoreType.DMA((2 * chunks + 6,)),
            pltpu.SemaphoreType.DMA((chunks + 5,)),
            pltpu.SemaphoreType.REGULAR,
        ],
        compiler_params=pltpu.CompilerParams(collective_id=0, has_side_effects=True),
        name="tracer_step",
    )(tracers, flat, kmt)
    return updated.reshape(tracers.shape)


def solution(mesh):
    return jax.shard_map(
        local,
        mesh=mesh,
        in_specs=(P(None, None, "lat", "lon"), P("lat", "lon")),
        out_specs=P(None, None, "lat", "lon"),
        check_vma=False,
    )
```

```python
import functools

import jax
import jax.numpy as jnp
from jax import lax
from jax.experimental import pallas as pl
from jax.experimental.pallas import tpu as pltpu
from jax.sharding import PartitionSpec as P

THERMAL = 0.2
HALINE = 0.8
REDI_COEF = 0.1
SKEW_COEF = 0.05
SLOPE_MAX = 0.6
SLOPE_WIDTH = 0.2
SLOPE_FLUX = (REDI_COEF - SKEW_COEF) * 0.25
CROSS = (REDI_COEF + SKEW_COEF) * 0.25 / REDI_COEF

ROWS = 8
LANES = 128
LEVELS = 8
SLAB = 16
MESH = pl.DeviceIdType.MESH
VMEM = pltpu.VMEM


def taper(slope):
    return slope * 0.5 * (1.0 + jnp.tanh((SLOPE_MAX - jnp.abs(slope)) / SLOPE_WIDTH))


def slope_of(step, mask, strat_twice):
    return taper(step * mask / jnp.maximum(0.25 * strat_twice, 1.0))


def below(limit, level):
    return jnp.where(level < limit, 1.0, 0.0)


def vertical_pair(values, mask, axis):
    size = values.shape[axis]
    diff = (pltpu.roll(values, size - 1, axis) - values) * mask
    return diff, diff + pltpu.roll(diff, 1, axis)


def tile(tracer, level):
    first = (tracer * LEVELS + level) * ROWS
    return pl.ds(first if isinstance(first, int) else pl.multiple_of(first, ROWS), ROWS)


def rows_of(tracer, row):
    return pl.ds(tracer * LEVELS * ROWS + row, LEVELS, stride=ROWS)


def up_one(values, axis):
    return pltpu.roll(values, values.shape[axis] - 1, axis)


def kernel(
    channels, chunks, early, tracers, flat, kmt, out,
    field, row_south, row_north, depth, from_south, from_north, depth_south, depth_north,
    sides, from_west, from_east,
    main, cross_x, coef, inner, edge, row_coef,
    load_sem, send_sem, recv_sem, ready,
):
    lon, lat = lax.axis_index("lon"), lax.axis_index("lat")
    blocks, bands = lax.axis_size("lon"), lax.axis_size("lat")
    top, bottom = lat == bands - 1, lat == 0
    west = (lax.rem(lon + blocks - 1, blocks), lat)
    east = (lax.rem(lon + 1, blocks), lat)
    north = (jnp.where(top, blocks - 1 - lon, lon), jnp.where(top, lat, lat + 1))
    south = (lon, jnp.maximum(lat - 1, 0))
    patient = jnp.logical_or(lax.rem(lon, SLAB) == 0, jnp.logical_and(top, lax.rem(lon, SLAB) < SLAB // 2 - 1))
    per_chunk = channels // chunks
    per_group = LANES // 2 // LEVELS
    groups = channels // per_group

    slab_at = lax.rem(lon, SLAB)
    opening = jnp.logical_and(slab_at == 0, jnp.logical_not(top))
    closing = jnp.logical_and(slab_at == SLAB - 1, jnp.logical_not(top))

    barrier = pltpu.get_barrier_semaphore()
    for other in (north, west):
        pl.semaphore_signal(barrier, inc=1, device_id=other, device_id_type=MESH)

    @pl.when(jnp.logical_not(closing))
    def _():
        pl.semaphore_signal(barrier, inc=1, device_id=east, device_id_type=MESH)

    @pl.when(jnp.logical_not(bottom))
    def _():
        pl.semaphore_signal(barrier, inc=1, device_id=south, device_id_type=MESH)

    rows_load = [
        pltpu.make_async_copy(tracers.at[:, :, ROWS - 1, :], row_north, load_sem.at[groups]),
        pltpu.make_async_copy(tracers.at[:, :, 0, :], row_south, load_sem.at[groups + 1]),
    ]
    depth_load = pltpu.make_async_copy(kmt, depth, load_sem.at[groups + 2])
    part = per_group * LEVELS * ROWS
    loads = [
        pltpu.make_async_copy(
            flat.at[pl.ds(group * part, part)], field.at[pl.ds(group * part, part)], load_sem.at[group]
        )
        for group in range(groups)
    ]
    depth_load.start()
    rows_load[0].start()
    for load in loads:
        load.start()
    rows_load[1].start()

    def send(source, target, slot, device, send_slot=None):
        return pltpu.make_async_remote_copy(
            src_ref=source,
            dst_ref=target,
            send_sem=send_sem.at[slot if send_slot is None else send_slot],
            recv_sem=recv_sem.at[slot],
            device_id=device,
            device_id_type=MESH,
        )

    def to_north_halo(own_row, values, device, first_send):
        copies = [send(depth.at[pl.ds(own_row, 1)], depth_north, 0, device, first_send)]
        for chunk in range(chunks):
            span = pl.ds(chunk * per_chunk, per_chunk)
            slot = 1 + chunk
            copies.append(send(values.at[span], from_north.at[span], slot, device, first_send + slot))
        return copies

    base = 1 + chunks
    fold = to_north_halo(ROWS - 1, row_north, north, base + 4)
    down = to_north_halo(0, row_south, south, 0)
    upward = [
        send(depth.at[pl.ds(ROWS - 1, 1)], depth_south, base, north),
        send(row_north, from_south, base + 1, north),
    ]
    across = [
        send(sides, from_east, base + 2, west),
        send(sides, from_west, base + 3, east),
    ]

    shape = (ROWS, LANES)
    lane = lax.broadcasted_iota(jnp.int32, shape, 1)
    row = lax.broadcasted_iota(jnp.int32, shape, 0)
    zero = jnp.zeros(shape, jnp.float32)

    def right(values, count=1):
        return pltpu.roll(values, count % LANES, 1)

    def wide(values):
        return jnp.broadcast_to(values, shape)

    pair_id = lax.rem(lane + 1, LANES) // 2
    at_edge = jnp.logical_or(lane == 0, lane == LANES - 1)

    def pack_columns():
        sides[groups] = depth[...].astype(jnp.float32)
        for group in range(groups):
            loads[group].wait()
            packed = zero
            for at in range(LANES // 2):
                tracer, k = group * per_group + at // LEVELS, at % LEVELS
                packed = jnp.where(pair_id == at, right(field[tile(tracer, k)], 2 * at), packed)
            sides[group] = packed

    def own_faces():
        depth_here = depth[...]
        density = [HALINE * field[tile(1, k)] - THERMAL * field[tile(0, k)] for k in range(LEVELS)]
        level_mask = [below(depth_here, k + 1) for k in range(LEVELS - 1)]
        strat_face = [(density[k + 1] - density[k]) * level_mask[k] for k in range(LEVELS - 1)]
        strat = [strat_face[0]]
        strat += [strat_face[k - 1] + strat_face[k] for k in range(1, LEVELS - 1)]
        strat += [strat_face[LEVELS - 2]]
        depth_left = jnp.minimum(depth_here, jnp.where(lane == 0, 0, right(depth_here)))
        depth_right = jnp.minimum(depth_here, jnp.where(lane == LANES - 1, 0, right(depth_here, -1)))
        depth_down = jnp.minimum(depth_here, jnp.where(row == 0, 0, pltpu.roll(depth_here, 1, 0)))
        inner_lanes = jnp.where(at_edge, 0.0, 1.0)
        inner_rows = jnp.where(jnp.logical_or(row == 0, row == ROWS - 1), 0.0, 1.0)
        sum_x, sum_y = [], []
        inner_slope = zero
        for k in range(LEVELS):
            mask_w, mask_e, mask_s = (below(limit, k) for limit in (depth_left, depth_right, depth_down))
            slope_w = slope_of(density[k] - right(density[k]), mask_w, strat[k] + right(strat[k]))
            slope_e = slope_of(right(density[k], -1) - density[k], mask_e, strat[k] + right(strat[k], -1))
            slope_s = slope_of(
                density[k] - pltpu.roll(density[k], 1, 0), mask_s, strat[k] + pltpu.roll(strat[k], 1, 0)
            )
            coef[0, k] = REDI_COEF * mask_w
            coef[1, k] = REDI_COEF * mask_e
            coef[2, k] = REDI_COEF * mask_s
            coef[3, k] = SLOPE_FLUX * slope_w
            coef[4, k] = SLOPE_FLUX * slope_e
            coef[5, k] = SLOPE_FLUX * slope_s
            coef[6, k] = level_mask[k] if k < LEVELS - 1 else zero
            sum_x.append(slope_w + slope_e)
            sum_y.append(slope_s + up_one(slope_s, 0))
            inner_slope = jnp.where(pair_id == k, right(sum_x[k], 2 * k), inner_slope)
            row_coef[0, pl.ds(k, 1)] = slope_s[1:2]
            row_coef[1, pl.ds(k, 1)] = REDI_COEF * mask_s[1:2]
            row_coef[2, pl.ds(k, 1)] = slope_s[ROWS - 1 : ROWS]
            row_coef[3, pl.ds(k, 1)] = REDI_COEF * mask_s[ROWS - 1 : ROWS]
        for k in range(LEVELS - 1):
            mean_x = 0.25 * (sum_x[k] + sum_x[k + 1]) * inner_lanes
            mean_y = 0.25 * (sum_y[k] + sum_y[k + 1]) * inner_rows
            coef[7, k] = CROSS * mean_x * level_mask[k]
            coef[8, k] = CROSS * mean_y * level_mask[k]
            coef[9, k] = REDI_COEF * (mean_x * mean_x + mean_y * mean_y)

        def one_group(group, carry):
            for slot in range(per_group):
                tracer = group * per_group + slot
                values = [field[tile(tracer, k)] for k in range(LEVELS)]
                diff = [(values[k + 1] - values[k]) * coef[6, k] for k in range(LEVELS - 1)]
                pair = [diff[0]] + [diff[k - 1] + diff[k] for k in range(1, LEVELS - 1)] + [diff[LEVELS - 2]]
                grad_x, grad_y, total = [], [], []
                for k in range(LEVELS):
                    here, both = values[k], pair[k]
                    grad_w = coef[0, k] * (here - right(here))
                    grad_e = coef[1, k] * (right(here, -1) - here)
                    grad_s = coef[2, k] * (here - pltpu.roll(here, 1, 0))
                    flux_w = grad_w + coef[3, k] * (both + right(both))
                    flux_e = grad_e + coef[4, k] * (both + right(both, -1))
                    flux_s = grad_s + coef[5, k] * (both + pltpu.roll(both, 1, 0))
                    grad_x.append(grad_w + grad_e)
                    grad_y.append(grad_s + up_one(grad_s, 0))
                    total.append(here + (flux_e - flux_w) + (up_one(flux_s, 0) - flux_s))
                above = None
                for k in range(LEVELS):
                    added = total[k] if above is None else total[k] - above
                    if k < LEVELS - 1:
                        both_x, both_y = grad_x[k] + grad_x[k + 1], grad_y[k] + grad_y[k + 1]
                        cross_x[tracer, k] = both_x
                        above = coef[7, k] * both_x + coef[8, k] * both_y + coef[9, k] * diff[k]
                        added = added + above
                    main[tile(tracer, k)] = added
            return carry

        coef[7, LEVELS - 1] = inner_slope
        lax.fori_loop(0, groups, one_group, 0)

        for group in range(groups):
            packed = zero
            for at in range(LANES // 2):
                tracer, k = group * per_group + at // LEVELS, at % LEVELS
                if k < LEVELS - 1:
                    packed = jnp.where(pair_id == at, right(cross_x[tracer, k], 2 * at), packed)
            inner[group] = packed

    def start_rows():
        for load in rows_load[1:]:
            load.wait()

        @pl.when(jnp.logical_not(bottom))
        def _():
            for copy in down:
                copy.start()

        @pl.when(jnp.logical_not(top))
        def _():
            for copy in upward:
                copy.start()

    def start_columns():
        across[1].start()
        pl.when(jnp.logical_not(opening))(across[0].start)

    def start_fold(copies):
        for copy in copies:
            copy.start()

    yielding = jnp.logical_and(top, jnp.logical_or(slab_at == SLAB - 4, slab_at == SLAB - 3))
    eager = jnp.logical_and(top, jnp.logical_not(jnp.logical_or(patient, yielding)))
    depth_load.wait()
    rows_load[0].wait()

    @pl.when(patient)
    def _():
        pack_columns()
        own_faces()

    pl.semaphore_wait(barrier, jnp.where(bottom, 3, 4) - jnp.where(opening, 1, 0))

    @pl.when(closing)
    def _():
        pl.semaphore_signal(ready, inc=1, device_id=east, device_id_type=MESH)

    @pl.when(patient)
    def _():
        start_rows()
        start_columns()
        pl.when(top)(functools.partial(start_fold, fold))

    @pl.when(jnp.logical_not(patient))
    def _():
        pl.when(eager)(functools.partial(start_fold, fold[:early]))
        pack_columns()
        start_columns()
        start_rows()
        pl.when(eager)(functools.partial(start_fold, fold[early:]))
        own_faces()
        pl.when(yielding)(functools.partial(start_fold, fold))

    @pl.when(bottom)
    def _():
        from_south[...] = jnp.zeros_like(from_south)
        depth_south[...] = jnp.zeros_like(depth_south)

    depth_here = depth[...]
    inner_slope = coef[7, LEVELS - 1]

    source_lane = jnp.where(top, LANES - 1 - lane, lane)

    def mirrored(values):
        return jnp.take_along_axis(values, source_lane, axis=1, mode="promise_in_bounds")

    def row_terms(at, own_row, beyond, depth_beyond, arranged, first):
        sign = 1.0 if at else -1.0
        beside_row = at - 1 if at else 1
        limit = wide(depth_here[at : at + 1])
        mask = below(limit, row + 1)
        limit_beyond = arranged(wide(depth_beyond[...]))
        mask_beyond = below(limit_beyond, row + 1)
        face = below(jnp.minimum(limit, limit_beyond), row)
        density_row = HALINE * own_row[1] - THERMAL * own_row[0]
        density_beyond = arranged(HALINE * beyond[1] - THERMAL * beyond[0])
        slope = slope_of(
            sign * (density_beyond - density_row),
            face,
            vertical_pair(density_row, mask, 0)[1] + vertical_pair(density_beyond, mask_beyond, 0)[1],
        )
        sums = slope + row_coef[first]
        mean = 0.25 * (sums + up_one(sums, 0))
        cross, square = CROSS * mean * mask, REDI_COEF * mean * mean
        grad_face, flux_face, grad_in = REDI_COEF * face, sign * SLOPE_FLUX * slope, row_coef[first + 1]

        def add(tracer, result):
            own, other = own_row[tracer], arranged(beyond[tracer])
            step = grad_face * (other - own)
            diff, pair = vertical_pair(own, mask, 0)
            both = pair + vertical_pair(other, mask_beyond, 0)[1]
            grads = sign * (step + grad_in * (own - field[rows_of(tracer, beside_row)]))
            vertical = cross * (grads + up_one(grads, 0)) + square * diff
            change = vertical - pltpu.roll(vertical, 1, 0) + (step + flux_face * both)
            result[rows_of(tracer, at)] = result[rows_of(tracer, at)] + change

        return add

    @pl.when(jnp.logical_not(bottom))
    def _():
        for copy in upward:
            copy.wait_recv()

    add_south = row_terms(0, row_south, from_south, depth_south, lambda values: values, 0)
    for tracer in range(channels):
        add_south(tracer, main)

    def north_face(result):
        for copy in down[:2]:
            copy.wait_recv()
        add_north = row_terms(ROWS - 1, row_north, from_north, depth_north, mirrored, 2)
        for chunk in range(chunks):
            if chunk:
                down[1 + chunk].wait_recv()
            for tracer in range(chunk * per_chunk, (chunk + 1) * per_chunk):
                add_north(tracer, result)

    pl.when(jnp.logical_not(top))(functools.partial(north_face, main))

    @pl.when(opening)
    def _():
        pl.semaphore_wait(ready, 1)
        across[0].start()

    even = lax.rem(lane, 2) == 0
    side_level = lax.rem(pair_id, LEVELS)
    side_sign = jnp.where(even, -1.0, 1.0)
    span = 2 * LEVELS

    def beside(group, shift=0):
        return jnp.where(even, right(from_west[group], 1 - shift), right(from_east[group], -1 - shift))

    def side_pair(values, mask):
        diff = (right(values, -2) - values) * mask
        return diff, diff + right(diff, 2)

    def every_tracer(values):
        values = jnp.where(pair_id < LEVELS, values, 0.0)
        total = values
        for shift in range(span, LANES, span):
            total = total + right(values, shift)
        return total

    here_limit = jnp.where(even, wide(depth_here[:, 0:1]), wide(depth_here[:, LANES - 1 : LANES]))
    here_mask = below(here_limit, side_level + 1)
    density_side = HALINE * right(sides[0], -span) - THERMAL * sides[0]
    strat_side = side_pair(density_side, here_mask)[1]

    for copy in across:
        copy.wait_recv()

    west_limit = wide(from_west[groups][:, LANES - 1 : LANES]).astype(jnp.int32)
    east_limit = wide(from_east[groups][:, 0:1]).astype(jnp.int32)
    there_limit = jnp.where(even, west_limit, east_limit)
    there_mask = below(there_limit, side_level + 1)
    side_mask = below(jnp.minimum(there_limit, here_limit), side_level)
    density_there = HALINE * beside(0, span) - THERMAL * beside(0)
    side_slope = slope_of(
        side_sign * (density_there - density_side),
        side_mask,
        strat_side + side_pair(density_there, there_mask)[1],
    )
    sums = side_slope + inner_slope
    mean = 0.25 * (sums + right(sums, -2))
    side_flux = every_tracer(SLOPE_FLUX * side_sign * side_slope)
    side_mean = every_tracer(mean)
    side_cross = CROSS * side_mean * here_mask
    side_square = REDI_COEF * side_mean * side_mean
    side_grad = REDI_COEF * side_mask
    for group in range(groups):
        own, other = sides[group], beside(group)
        step = side_grad * (other - own)
        diff, pair = side_pair(own, here_mask)
        grads = inner[group] + side_sign * (step + right(step, -2))
        vertical = side_cross * grads + side_square * diff
        change = vertical - right(vertical, 2) + step + side_flux * (pair + side_pair(other, there_mask)[1])
        edge[group] = change
    for group in range(groups):
        change = edge[group]
        for at in range(LANES // 2):
            tracer, k = group * per_group + at // LEVELS, at % LEVELS
            out[tile(tracer, k)] = main[tile(tracer, k)] + jnp.where(at_edge, right(change, -2 * at), 0.0)

    pl.when(top)(functools.partial(north_face, out))

    for copy in across:
        copy.wait_send()

    @pl.when(top)
    def _():
        for copy in fold:
            copy.wait_send()

    @pl.when(jnp.logical_not(top))
    def _():
        for copy in upward:
            copy.wait_send()

    @pl.when(jnp.logical_not(bottom))
    def _():
        for copy in down:
            copy.wait_send()


def local(tracers, kmt):
    channels = tracers.shape[0]
    chunks = 4
    early = 2
    groups = channels * LEVELS * 2 // LANES
    row_array = VMEM((channels, LEVELS, LANES), jnp.float32)
    packed = VMEM((groups + 1, ROWS, LANES), jnp.float32)
    depth_row = VMEM((1, LANES), jnp.int32)
    anywhere = pl.BlockSpec(memory_space=pl.ANY)
    flat = tracers.reshape(-1, LANES)
    updated = pl.pallas_call(
        functools.partial(kernel, channels, chunks, early),
        out_shape=VMEM(flat.shape, jnp.float32),
        in_specs=[anywhere, anywhere, anywhere],
        out_specs=pl.BlockSpec(memory_space=VMEM),
        scratch_shapes=[
            VMEM(flat.shape, jnp.float32),
            row_array, row_array, VMEM((ROWS, LANES), jnp.int32),
            row_array, row_array, depth_row, depth_row,
            packed, packed, packed,
            VMEM(flat.shape, jnp.float32),
            VMEM((channels, LEVELS - 1, ROWS, LANES), jnp.float32),
            VMEM((10, LEVELS, ROWS, LANES), jnp.float32),
            VMEM((groups, ROWS, LANES), jnp.float32),
            VMEM((groups, ROWS, LANES), jnp.float32),
            VMEM((4, LEVELS, LANES), jnp.float32),
            pltpu.SemaphoreType.DMA((groups + 3,)),
            pltpu.SemaphoreType.DMA((2 * chunks + 6,)),
            pltpu.SemaphoreType.DMA((chunks + 5,)),
            pltpu.SemaphoreType.REGULAR,
        ],
        compiler_params=pltpu.CompilerParams(collective_id=0, has_side_effects=True),
        name="tracer_step",
    )(tracers, flat, kmt)
    return updated.reshape(tracers.shape)


def solution(mesh):
    return jax.shard_map(
        local,
        mesh=mesh,
        in_specs=(P(None, None, "lat", "lon"), P("lat", "lon")),
        out_specs=P(None, None, "lat", "lon"),
        check_vma=False,
    )
```

```python
import functools

import jax
import jax.numpy as jnp
from jax import lax
from jax.experimental import pallas as pl
from jax.experimental.pallas import tpu as pltpu
from jax.sharding import PartitionSpec as P

THERMAL = 0.2
HALINE = 0.8
REDI_COEF = 0.1
SKEW_COEF = 0.05
SLOPE_MAX = 0.6
SLOPE_WIDTH = 0.2
SLOPE_FLUX = (REDI_COEF - SKEW_COEF) * 0.25
CROSS = (REDI_COEF + SKEW_COEF) * 0.25 / REDI_COEF

ROWS = 8
LANES = 128
LEVELS = 8
SLAB = 16
MESH = pl.DeviceIdType.MESH
VMEM = pltpu.VMEM


def taper(slope):
    return slope * 0.5 * (1.0 + jnp.tanh((SLOPE_MAX - jnp.abs(slope)) / SLOPE_WIDTH))


def slope_of(step, mask, strat_twice):
    return taper(step * mask / jnp.maximum(0.25 * strat_twice, 1.0))


def below(limit, level):
    return jnp.where(level < limit, 1.0, 0.0)


def vertical_pair(values, mask, axis):
    size = values.shape[axis]
    diff = (pltpu.roll(values, size - 1, axis) - values) * mask
    return diff, diff + pltpu.roll(diff, 1, axis)


def tile(tracer, level):
    first = (tracer * LEVELS + level) * ROWS
    return pl.ds(first if isinstance(first, int) else pl.multiple_of(first, ROWS), ROWS)


def rows_of(tracer, row):
    return pl.ds(tracer * LEVELS * ROWS + row, LEVELS, stride=ROWS)


def up_one(values, axis):
    return pltpu.roll(values, values.shape[axis] - 1, axis)


def kernel(
    channels, chunks, early, tracers, flat, kmt, out,
    field, row_south, row_north, depth, from_south, from_north, depth_south, depth_north,
    sides, from_west, from_east,
    main, cross_x, coef, inner, edge, row_coef,
    load_sem, send_sem, recv_sem, ready,
):
    lon, lat = lax.axis_index("lon"), lax.axis_index("lat")
    blocks, bands = lax.axis_size("lon"), lax.axis_size("lat")
    top, bottom = lat == bands - 1, lat == 0
    west = (lax.rem(lon + blocks - 1, blocks), lat)
    east = (lax.rem(lon + 1, blocks), lat)
    north = (jnp.where(top, blocks - 1 - lon, lon), jnp.where(top, lat, lat + 1))
    south = (lon, jnp.maximum(lat - 1, 0))
    patient = jnp.logical_or(lax.rem(lon, SLAB) == 0, jnp.logical_and(top, lax.rem(lon, SLAB) < SLAB // 2 - 1))
    per_chunk = channels // chunks
    per_group = LANES // 2 // LEVELS
    groups = channels // per_group

    slab_at = lax.rem(lon, SLAB)
    opening = jnp.logical_and(slab_at == 0, jnp.logical_not(top))
    closing = jnp.logical_and(slab_at == SLAB - 1, jnp.logical_not(top))

    barrier = pltpu.get_barrier_semaphore()
    for other in (north, west):
        pl.semaphore_signal(barrier, inc=1, device_id=other, device_id_type=MESH)

    @pl.when(jnp.logical_not(closing))
    def _():
        pl.semaphore_signal(barrier, inc=1, device_id=east, device_id_type=MESH)

    @pl.when(jnp.logical_not(bottom))
    def _():
        pl.semaphore_signal(barrier, inc=1, device_id=south, device_id_type=MESH)

    rows_load = [
        pltpu.make_async_copy(tracers.at[:, :, ROWS - 1, :], row_north, load_sem.at[groups]),
        pltpu.make_async_copy(tracers.at[:, :, 0, :], row_south, load_sem.at[groups + 1]),
    ]
    depth_load = pltpu.make_async_copy(kmt, depth, load_sem.at[groups + 2])
    part = per_group * LEVELS * ROWS
    loads = [
        pltpu.make_async_copy(
            flat.at[pl.ds(group * part, part)], field.at[pl.ds(group * part, part)], load_sem.at[group]
        )
        for group in range(groups)
    ]
    depth_load.start()
    rows_load[0].start()
    for load in loads:
        load.start()
    rows_load[1].start()

    def send(source, target, slot, device, send_slot=None):
        return pltpu.make_async_remote_copy(
            src_ref=source,
            dst_ref=target,
            send_sem=send_sem.at[slot if send_slot is None else send_slot],
            recv_sem=recv_sem.at[slot],
            device_id=device,
            device_id_type=MESH,
        )

    def to_north_halo(own_row, values, device, first_send):
        copies = [send(depth.at[pl.ds(own_row, 1)], depth_north, 0, device, first_send)]
        for chunk in range(chunks):
            span = pl.ds(chunk * per_chunk, per_chunk)
            slot = 1 + chunk
            copies.append(send(values.at[span], from_north.at[span], slot, device, first_send + slot))
        return copies

    base = 1 + chunks
    fold = to_north_halo(ROWS - 1, row_north, north, base + 4)
    down = to_north_halo(0, row_south, south, 0)
    upward = [
        send(depth.at[pl.ds(ROWS - 1, 1)], depth_south, base, north),
        send(row_north, from_south, base + 1, north),
    ]
    across = [
        send(sides, from_east, base + 2, west),
        send(sides, from_west, base + 3, east),
    ]

    shape = (ROWS, LANES)
    lane = lax.broadcasted_iota(jnp.int32, shape, 1)
    row = lax.broadcasted_iota(jnp.int32, shape, 0)
    zero = jnp.zeros(shape, jnp.float32)

    def right(values, count=1):
        return pltpu.roll(values, count % LANES, 1)

    def wide(values):
        return jnp.broadcast_to(values, shape)

    pair_id = lax.rem(lane + 1, LANES) // 2
    at_edge = jnp.logical_or(lane == 0, lane == LANES - 1)

    def pack_columns():
        sides[groups] = depth[...].astype(jnp.float32)
        for group in range(groups):
            loads[group].wait()
            packed = zero
            for at in range(LANES // 2):
                tracer, k = group * per_group + at // LEVELS, at % LEVELS
                packed = jnp.where(pair_id == at, right(field[tile(tracer, k)], 2 * at), packed)
            sides[group] = packed

    def own_faces():
        depth_here = depth[...]
        density = [HALINE * field[tile(1, k)] - THERMAL * field[tile(0, k)] for k in range(LEVELS)]
        level_mask = [below(depth_here, k + 1) for k in range(LEVELS - 1)]
        strat_face = [(density[k + 1] - density[k]) * level_mask[k] for k in range(LEVELS - 1)]
        strat = [strat_face[0]]
        strat += [strat_face[k - 1] + strat_face[k] for k in range(1, LEVELS - 1)]
        strat += [strat_face[LEVELS - 2]]
        depth_left = jnp.minimum(depth_here, jnp.where(lane == 0, 0, right(depth_here)))
        depth_right = jnp.minimum(depth_here, jnp.where(lane == LANES - 1, 0, right(depth_here, -1)))
        depth_down = jnp.minimum(depth_here, jnp.where(row == 0, 0, pltpu.roll(depth_here, 1, 0)))
        inner_lanes = jnp.where(at_edge, 0.0, 1.0)
        inner_rows = jnp.where(jnp.logical_or(row == 0, row == ROWS - 1), 0.0, 1.0)
        sum_x, sum_y = [], []
        inner_slope = zero
        for k in range(LEVELS):
            mask_w, mask_e, mask_s = (below(limit, k) for limit in (depth_left, depth_right, depth_down))
            slope_w = slope_of(density[k] - right(density[k]), mask_w, strat[k] + right(strat[k]))
            slope_e = slope_of(right(density[k], -1) - density[k], mask_e, strat[k] + right(strat[k], -1))
            slope_s = slope_of(
                density[k] - pltpu.roll(density[k], 1, 0), mask_s, strat[k] + pltpu.roll(strat[k], 1, 0)
            )
            coef[0, k] = REDI_COEF * mask_w
            coef[1, k] = REDI_COEF * mask_e
            coef[2, k] = REDI_COEF * mask_s
            coef[3, k] = SLOPE_FLUX * slope_w
            coef[4, k] = SLOPE_FLUX * slope_e
            coef[5, k] = SLOPE_FLUX * slope_s
            coef[6, k] = level_mask[k] if k < LEVELS - 1 else zero
            sum_x.append(slope_w + slope_e)
            sum_y.append(slope_s + up_one(slope_s, 0))
            inner_slope = jnp.where(pair_id == k, right(sum_x[k], 2 * k), inner_slope)
            row_coef[0, pl.ds(k, 1)] = slope_s[1:2]
            row_coef[1, pl.ds(k, 1)] = REDI_COEF * mask_s[1:2]
            row_coef[2, pl.ds(k, 1)] = slope_s[ROWS - 1 : ROWS]
            row_coef[3, pl.ds(k, 1)] = REDI_COEF * mask_s[ROWS - 1 : ROWS]
        for k in range(LEVELS - 1):
            mean_x = 0.25 * (sum_x[k] + sum_x[k + 1]) * inner_lanes
            mean_y = 0.25 * (sum_y[k] + sum_y[k + 1]) * inner_rows
            coef[7, k] = CROSS * mean_x * level_mask[k]
            coef[8, k] = CROSS * mean_y * level_mask[k]
            coef[9, k] = REDI_COEF * (mean_x * mean_x + mean_y * mean_y)

        def one_group(group, carry):
            for slot in range(per_group):
                tracer = group * per_group + slot
                values = [field[tile(tracer, k)] for k in range(LEVELS)]
                diff = [(values[k + 1] - values[k]) * coef[6, k] for k in range(LEVELS - 1)]
                pair = [diff[0]] + [diff[k - 1] + diff[k] for k in range(1, LEVELS - 1)] + [diff[LEVELS - 2]]
                grad_x, grad_y, total = [], [], []
                for k in range(LEVELS):
                    here, both = values[k], pair[k]
                    grad_w = coef[0, k] * (here - right(here))
                    grad_e = coef[1, k] * (right(here, -1) - here)
                    grad_s = coef[2, k] * (here - pltpu.roll(here, 1, 0))
                    flux_w = grad_w + coef[3, k] * (both + right(both))
                    flux_e = grad_e + coef[4, k] * (both + right(both, -1))
                    flux_s = grad_s + coef[5, k] * (both + pltpu.roll(both, 1, 0))
                    grad_x.append(grad_w + grad_e)
                    grad_y.append(grad_s + up_one(grad_s, 0))
                    total.append(here + (flux_e - flux_w) + (up_one(flux_s, 0) - flux_s))
                above = None
                for k in range(LEVELS):
                    added = total[k] if above is None else total[k] - above
                    if k < LEVELS - 1:
                        both_x, both_y = grad_x[k] + grad_x[k + 1], grad_y[k] + grad_y[k + 1]
                        cross_x[tracer, k] = both_x
                        above = coef[7, k] * both_x + coef[8, k] * both_y + coef[9, k] * diff[k]
                        added = added + above
                    main[tile(tracer, k)] = added
            return carry

        coef[7, LEVELS - 1] = inner_slope
        lax.fori_loop(0, groups, one_group, 0)

    def pack_sums():
        for group in range(groups):
            packed = zero
            for at in range(LANES // 2):
                tracer, k = group * per_group + at // LEVELS, at % LEVELS
                if k < LEVELS - 1:
                    packed = jnp.where(pair_id == at, right(cross_x[tracer, k], 2 * at), packed)
            inner[group] = packed

    def start_rows():
        for load in rows_load[1:]:
            load.wait()

        @pl.when(jnp.logical_not(bottom))
        def _():
            for copy in down:
                copy.start()

        @pl.when(jnp.logical_not(top))
        def _():
            for copy in upward:
                copy.start()

    def start_columns():
        across[1].start()
        pl.when(jnp.logical_not(opening))(across[0].start)

    def start_fold(copies):
        for copy in copies:
            copy.start()

    yielding = jnp.logical_and(top, jnp.logical_or(slab_at == SLAB - 4, slab_at == SLAB - 3))
    eager = jnp.logical_and(top, jnp.logical_not(jnp.logical_or(patient, yielding)))
    depth_load.wait()
    rows_load[0].wait()

    @pl.when(patient)
    def _():
        pack_columns()
        own_faces()
        pack_sums()

    pl.semaphore_wait(barrier, jnp.where(bottom, 3, 4) - jnp.where(opening, 1, 0))

    @pl.when(closing)
    def _():
        pl.semaphore_signal(ready, inc=1, device_id=east, device_id_type=MESH)

    @pl.when(patient)
    def _():
        start_rows()
        start_columns()
        pl.when(top)(functools.partial(start_fold, fold))

    @pl.when(jnp.logical_not(patient))
    def _():
        pl.when(eager)(functools.partial(start_fold, fold[:early]))
        pack_columns()
        start_columns()
        start_rows()
        pl.when(eager)(functools.partial(start_fold, fold[early:]))
        own_faces()
        pl.when(yielding)(functools.partial(start_fold, fold))
        pack_sums()

    @pl.when(bottom)
    def _():
        from_south[...] = jnp.zeros_like(from_south)
        depth_south[...] = jnp.zeros_like(depth_south)

    depth_here = depth[...]
    inner_slope = coef[7, LEVELS - 1]

    source_lane = jnp.where(top, LANES - 1 - lane, lane)

    def mirrored(values):
        return jnp.take_along_axis(values, source_lane, axis=1, mode="promise_in_bounds")

    def row_terms(at, own_row, beyond, depth_beyond, arranged, first):
        sign = 1.0 if at else -1.0
        beside_row = at - 1 if at else 1
        limit = wide(depth_here[at : at + 1])
        mask = below(limit, row + 1)
        limit_beyond = arranged(wide(depth_beyond[...]))
        mask_beyond = below(limit_beyond, row + 1)
        face = below(jnp.minimum(limit, limit_beyond), row)
        density_row = HALINE * own_row[1] - THERMAL * own_row[0]
        density_beyond = arranged(HALINE * beyond[1] - THERMAL * beyond[0])
        slope = slope_of(
            sign * (density_beyond - density_row),
            face,
            vertical_pair(density_row, mask, 0)[1] + vertical_pair(density_beyond, mask_beyond, 0)[1],
        )
        sums = slope + row_coef[first]
        mean = 0.25 * (sums + up_one(sums, 0))
        cross, square = CROSS * mean * mask, REDI_COEF * mean * mean
        grad_face, flux_face, grad_in = REDI_COEF * face, sign * SLOPE_FLUX * slope, row_coef[first + 1]

        def add(tracer, result):
            own, other = own_row[tracer], arranged(beyond[tracer])
            step = grad_face * (other - own)
            diff, pair = vertical_pair(own, mask, 0)
            both = pair + vertical_pair(other, mask_beyond, 0)[1]
            grads = sign * (step + grad_in * (own - field[rows_of(tracer, beside_row)]))
            vertical = cross * (grads + up_one(grads, 0)) + square * diff
            change = vertical - pltpu.roll(vertical, 1, 0) + (step + flux_face * both)
            result[rows_of(tracer, at)] = result[rows_of(tracer, at)] + change

        return add

    @pl.when(jnp.logical_not(bottom))
    def _():
        for copy in upward:
            copy.wait_recv()

    add_south = row_terms(0, row_south, from_south, depth_south, lambda values: values, 0)
    for tracer in range(channels):
        add_south(tracer, main)

    def north_face(result):
        for copy in down[:2]:
            copy.wait_recv()
        add_north = row_terms(ROWS - 1, row_north, from_north, depth_north, mirrored, 2)
        for chunk in range(chunks):
            if chunk:
                down[1 + chunk].wait_recv()
            for tracer in range(chunk * per_chunk, (chunk + 1) * per_chunk):
                add_north(tracer, result)

    pl.when(jnp.logical_not(top))(functools.partial(north_face, main))

    @pl.when(opening)
    def _():
        pl.semaphore_wait(ready, 1)
        across[0].start()

    even = lax.rem(lane, 2) == 0
    side_level = lax.rem(pair_id, LEVELS)
    side_sign = jnp.where(even, -1.0, 1.0)
    span = 2 * LEVELS

    def beside(group, shift=0):
        return jnp.where(even, right(from_west[group], 1 - shift), right(from_east[group], -1 - shift))

    def side_pair(values, mask):
        diff = (right(values, -2) - values) * mask
        return diff, diff + right(diff, 2)

    def every_tracer(values):
        values = jnp.where(pair_id < LEVELS, values, 0.0)
        total = values
        for shift in range(span, LANES, span):
            total = total + right(values, shift)
        return total

    here_limit = jnp.where(even, wide(depth_here[:, 0:1]), wide(depth_here[:, LANES - 1 : LANES]))
    here_mask = below(here_limit, side_level + 1)
    density_side = HALINE * right(sides[0], -span) - THERMAL * sides[0]
    strat_side = side_pair(density_side, here_mask)[1]

    for copy in across:
        copy.wait_recv()

    west_limit = wide(from_west[groups][:, LANES - 1 : LANES]).astype(jnp.int32)
    east_limit = wide(from_east[groups][:, 0:1]).astype(jnp.int32)
    there_limit = jnp.where(even, west_limit, east_limit)
    there_mask = below(there_limit, side_level + 1)
    side_mask = below(jnp.minimum(there_limit, here_limit), side_level)
    density_there = HALINE * beside(0, span) - THERMAL * beside(0)
    side_slope = slope_of(
        side_sign * (density_there - density_side),
        side_mask,
        strat_side + side_pair(density_there, there_mask)[1],
    )
    sums = side_slope + inner_slope
    mean = 0.25 * (sums + right(sums, -2))
    side_flux = every_tracer(SLOPE_FLUX * side_sign * side_slope)
    side_mean = every_tracer(mean)
    side_cross = CROSS * side_mean * here_mask
    side_square = REDI_COEF * side_mean * side_mean
    side_grad = REDI_COEF * side_mask
    for group in range(groups):
        own, other = sides[group], beside(group)
        step = side_grad * (other - own)
        diff, pair = side_pair(own, here_mask)
        grads = inner[group] + side_sign * (step + right(step, -2))
        vertical = side_cross * grads + side_square * diff
        change = vertical - right(vertical, 2) + step + side_flux * (pair + side_pair(other, there_mask)[1])
        edge[group] = change
    for group in range(groups):
        change = edge[group]
        for at in range(LANES // 2):
            tracer, k = group * per_group + at // LEVELS, at % LEVELS
            out[tile(tracer, k)] = main[tile(tracer, k)] + jnp.where(at_edge, right(change, -2 * at), 0.0)

    pl.when(top)(functools.partial(north_face, out))

    for copy in across:
        copy.wait_send()

    @pl.when(top)
    def _():
        for copy in fold:
            copy.wait_send()

    @pl.when(jnp.logical_not(top))
    def _():
        for copy in upward:
            copy.wait_send()

    @pl.when(jnp.logical_not(bottom))
    def _():
        for copy in down:
            copy.wait_send()


def local(tracers, kmt):
    channels = tracers.shape[0]
    chunks = 4
    early = 2
    groups = channels * LEVELS * 2 // LANES
    row_array = VMEM((channels, LEVELS, LANES), jnp.float32)
    packed = VMEM((groups + 1, ROWS, LANES), jnp.float32)
    depth_row = VMEM((1, LANES), jnp.int32)
    anywhere = pl.BlockSpec(memory_space=pl.ANY)
    flat = tracers.reshape(-1, LANES)
    updated = pl.pallas_call(
        functools.partial(kernel, channels, chunks, early),
        out_shape=VMEM(flat.shape, jnp.float32),
        in_specs=[anywhere, anywhere, anywhere],
        out_specs=pl.BlockSpec(memory_space=VMEM),
        scratch_shapes=[
            VMEM(flat.shape, jnp.float32),
            row_array, row_array, VMEM((ROWS, LANES), jnp.int32),
            row_array, row_array, depth_row, depth_row,
            packed, packed, packed,
            VMEM(flat.shape, jnp.float32),
            VMEM((channels, LEVELS - 1, ROWS, LANES), jnp.float32),
            VMEM((10, LEVELS, ROWS, LANES), jnp.float32),
            VMEM((groups, ROWS, LANES), jnp.float32),
            VMEM((groups, ROWS, LANES), jnp.float32),
            VMEM((4, LEVELS, LANES), jnp.float32),
            pltpu.SemaphoreType.DMA((groups + 3,)),
            pltpu.SemaphoreType.DMA((2 * chunks + 6,)),
            pltpu.SemaphoreType.DMA((chunks + 5,)),
            pltpu.SemaphoreType.REGULAR,
        ],
        compiler_params=pltpu.CompilerParams(collective_id=0, has_side_effects=True),
        name="tracer_step",
    )(tracers, flat, kmt)
    return updated.reshape(tracers.shape)


def solution(mesh):
    return jax.shard_map(
        local,
        mesh=mesh,
        in_specs=(P(None, None, "lat", "lon"), P("lat", "lon")),
        out_specs=P(None, None, "lat", "lon"),
        check_vma=False,
    )
```
